32 devices in a mesh: dp: 2 (over x), tp: 4 (over z), sp: 4 (over y, core).
Axes of the slice: x: 2, y: 2, z: 4, core: 2. Of those that a mesh axis runs over, the one named last changes fastest.
Arguments:
- tokens: bfloat16 [128, 2560], P('dp'), parts along dimension 0
- positions: int32 [128], P('dp'), parts along dimension 0
- cache_k: bfloat16 [128, 1024, 4, 256], P('dp', 'sp', 'tp'), parts along dimension 0
- cache_v: bfloat16 [128, 1024, 4, 256], P('dp', 'sp', 'tp'), parts along dimension 0
- attn_gain: bfloat16 [2560], replicated
- w_q: bfloat16 [2560, 2048], P(None, 'tp')
- w_k: bfloat16 [2560, 1024], P(None, 'tp')
- w_v: bfloat16 [2560, 1024], P(None, 'tp')
- w_o: bfloat16 [2048, 2560], P('tp')
- mlp_gain: bfloat16 [2560], replicated
- w_gate: bfloat16 [2560, 10240], P(None, 'tp')
- w_up: bfloat16 [2560, 10240], P(None, 'tp')
- w_down: bfloat16 [10240, 2560], P('tp')
Outputs:
- output 1: bfloat16 [128, 2560], P('dp'), parts along dimension 0
- output 2: bfloat16 [128, 1024, 4, 256], P('dp', 'sp', 'tp'), parts along dimension 0
- output 3: bfloat16 [128, 1024, 4, 256], P('dp', 'sp', 'tp'), parts along dimension 0
There are 2 independent parts. The reference program is written for one: setup_inputs(seed, part) draws one part's arguments, and reference() takes and returns one part's arrays. A program takes and returns all parts, laid end to end along the dimension named above; an argument that names none is the same for every part.
All inputs are finite; a program needn't handle non-finite values.
Results may differ from the reference program's by a relative error of at most 0.00832149.
Values sent between devices are 32-bit elements.
A program may use at most 1 GiB of HBM per device.

```python
import math
import jax
import jax.numpy as jnp
from jax import lax

BATCH = 64
MODEL_DIM = 2560
HEADS = 8
KV_HEADS = 4
HEAD_DIM = 256
MLP_DIM = 10240
SLOTS = 1024
GROUP = HEADS // KV_HEADS
POS_LIMIT = 8 * SLOTS
LOG_SLOTS = int(math.log2(SLOTS))
NORM_EPS = 1e-5
ROPE_THETA = 10000.0
KEY_STD = math.sqrt(math.log(SLOTS / 8.0))
VALUE_STD = 1.5


def draw_positions(key):
    rank_key, scale_key, young_key, old_key = jax.random.split(key, 4)
    order = jax.random.permutation(rank_key, BATCH)
    is_young = order < BATCH // 2
    exponent = jax.random.randint(scale_key, (BATCH,), 0, LOG_SLOTS + 1)
    limit = jnp.minimum(jnp.left_shift(jnp.ones_like(exponent), exponent), SLOTS)
    young_pos = jax.random.randint(young_key, (BATCH,), 0, limit)
    old_pos = jax.random.randint(old_key, (BATCH,), SLOTS, POS_LIMIT)
    return jnp.where(is_young, young_pos, old_pos).astype(jnp.int32)


def normal_matrix(key, rows, columns, scale):
    return (jax.random.normal(key, (rows, columns), jnp.float32) * scale).astype(jnp.bfloat16)


def normal_gain(key):
    return (1.0 + 0.3 * jax.random.normal(key, (MODEL_DIM,), jnp.float32)).astype(jnp.bfloat16)


def setup_inputs(seed: int = 0, part: int = 0) -> dict:
    base_key = jax.random.key(seed)
    part_keys = jax.random.split(jax.random.fold_in(base_key, part), 4)
    weight_keys = jax.random.split(base_key, 9)
    cache_shape = (BATCH, SLOTS, KV_HEADS, HEAD_DIM)
    query_width = HEADS * HEAD_DIM
    kv_width = KV_HEADS * HEAD_DIM
    tokens = jax.random.normal(part_keys[0], (BATCH, MODEL_DIM), jnp.float32).astype(jnp.bfloat16)
    positions = draw_positions(part_keys[1])
    cache_k = (KEY_STD * jax.random.normal(part_keys[2], cache_shape, jnp.float32)).astype(jnp.bfloat16)
    cache_v = (VALUE_STD * jax.random.normal(part_keys[3], cache_shape, jnp.float32)).astype(jnp.bfloat16)
    return {
        "tokens": tokens,
        "positions": positions,
        "cache_k": cache_k,
        "cache_v": cache_v,
        "attn_gain": normal_gain(weight_keys[0]),
        "w_q": normal_matrix(weight_keys[1], MODEL_DIM, query_width, MODEL_DIM ** -0.5),
        "w_k": normal_matrix(weight_keys[2], MODEL_DIM, kv_width, KEY_STD * MODEL_DIM ** -0.5),
        "w_v": normal_matrix(weight_keys[3], MODEL_DIM, kv_width, VALUE_STD * MODEL_DIM ** -0.5),
        "w_o": normal_matrix(weight_keys[4], query_width, MODEL_DIM, query_width ** -0.5),
        "mlp_gain": normal_gain(weight_keys[5]),
        "w_gate": normal_matrix(weight_keys[6], MODEL_DIM, MLP_DIM, MODEL_DIM ** -0.5),
        "w_up": normal_matrix(weight_keys[7], MODEL_DIM, MLP_DIM, MODEL_DIM ** -0.5),
        "w_down": normal_matrix(weight_keys[8], MLP_DIM, MODEL_DIM, MLP_DIM ** -0.5),
    }


def rms_norm(values, gain):
    wide = values.astype(jnp.float32)
    inv_rms = lax.rsqrt(jnp.mean(wide * wide, axis=-1, keepdims=True) + NORM_EPS)
    return (wide * inv_rms * gain.astype(jnp.float32)).astype(jnp.bfloat16)


def rope_tables(positions):
    frequencies = ROPE_THETA ** (-2.0 * jnp.arange(HEAD_DIM // 2, dtype=jnp.float32) / HEAD_DIM)
    angles = positions.astype(jnp.float32)[:, None] * frequencies[None, :]
    return jnp.cos(angles)[:, None, :], jnp.sin(angles)[:, None, :]


def apply_rope(vectors, cos_table, sin_table):
    half = vectors.shape[-1] // 2
    first = vectors[..., :half]
    second = vectors[..., half:]
    return jnp.concatenate([first * cos_table - second * sin_table, second * cos_table + first * sin_table], axis=-1)


def reference(tokens, positions, cache_k, cache_v, attn_gain, w_q, w_k, w_v, w_o, mlp_gain, w_gate, w_up, w_down):
    normed = rms_norm(tokens, attn_gain)
    cos_table, sin_table = rope_tables(positions)
    q_lin = jnp.dot(normed, w_q, preferred_element_type=jnp.float32).reshape(BATCH, HEADS, HEAD_DIM)
    k_lin = jnp.dot(normed, w_k, preferred_element_type=jnp.float32).reshape(BATCH, KV_HEADS, HEAD_DIM)
    v_new = jnp.dot(normed, w_v, preferred_element_type=jnp.float32).astype(jnp.bfloat16).reshape(BATCH, KV_HEADS, HEAD_DIM)
    q_rot = apply_rope(q_lin, cos_table, sin_table).astype(jnp.bfloat16)
    k_rot = apply_rope(k_lin, cos_table, sin_table).astype(jnp.bfloat16)
    slot_ids = jnp.arange(SLOTS)
    hit_mask = (slot_ids[None, :] == (positions % SLOTS)[:, None])[:, :, None, None]
    new_k = jnp.where(hit_mask, k_rot[:, None], cache_k)
    new_v = jnp.where(hit_mask, v_new[:, None], cache_v)

    def attend_one(item):
        q_seq, k_seq, v_seq, pos_one = item
        query = q_seq.astype(jnp.float32).reshape(KV_HEADS, GROUP, HEAD_DIM)
        scores = jnp.einsum("kgd,skd->kgs", query, k_seq.astype(jnp.float32)) / math.sqrt(HEAD_DIM)
        valid = (pos_one >= SLOTS - 1) | (slot_ids <= pos_one)
        scores = jnp.where(valid[None, None, :], scores, -jnp.inf)
        weights = jax.nn.softmax(scores, axis=-1)
        return jnp.einsum("kgs,skd->kgd", weights, v_seq.astype(jnp.float32)).reshape(HEADS, HEAD_DIM)

    attended = lax.map(attend_one, (q_rot, new_k, new_v, positions))
    attended = attended.reshape(BATCH, HEADS * HEAD_DIM).astype(jnp.bfloat16)
    attn_proj = jnp.dot(attended, w_o, preferred_element_type=jnp.float32)
    hidden = (tokens.astype(jnp.float32) + attn_proj).astype(jnp.bfloat16)
    normed_mlp = rms_norm(hidden, mlp_gain)
    gate_proj = jnp.dot(normed_mlp, w_gate, preferred_element_type=jnp.float32)
    up_proj = jnp.dot(normed_mlp, w_up, preferred_element_type=jnp.float32)
    activated = (jax.nn.silu(gate_proj) * up_proj).astype(jnp.bfloat16)
    mlp_down = jnp.dot(activated, w_down, preferred_element_type=jnp.float32)
    layer_out = (hidden.astype(jnp.float32) + mlp_down).astype(jnp.bfloat16)
    return (layer_out, new_k, new_v)
```

```python
import functools
import math

import jax
import jax.numpy as jnp
import numpy as np
from jax import lax
from jax.experimental import pallas as pl
from jax.experimental.pallas import tpu as pltpu
from jax.sharding import PartitionSpec as P

NORM_EPS = 1e-5
ROPE_THETA = 10000.0
F32 = jnp.float32
BF16 = jnp.bfloat16
CHUNK = 16


def rms_norm(values, gain):
    wide = values.astype(F32)
    inv_rms = lax.rsqrt(jnp.mean(wide * wide, axis=-1, keepdims=True) + NORM_EPS)
    return (wide * inv_rms * gain.astype(F32)).astype(BF16)


def attn_kernel(sp_size, pos_ref, freq_ref, tok_hbm, gain_hbm, wq_hbm, wk_hbm, wv_hbm, ck_hbm, cv_hbm,
                nk_hbm, nv_hbm, part_ref, nk_ref, nv_ref, tok, gain, wq, wk, wv, qs, knew, vnew, posm,
                sem_w, sem_k, sem_v, sem_ko, sem_vo):
    rows = tok.shape[0]
    local_slots = nk_ref.shape[1]
    dim = nk_ref.shape[2]
    half = dim // 2
    slots = local_slots * sp_size
    chunks = rows // CHUNK
    base = lax.axis_index("sp") * local_slots

    loads = [pltpu.make_async_copy(src, dst, sem_w.at[i]) for i, (src, dst) in enumerate(
        ((tok_hbm, tok), (gain_hbm, gain), (wk_hbm, wk), (wv_hbm, wv), (wq_hbm, wq)))]
    for copy in loads:
        copy.start()
    k_loads, v_loads, k_stores, v_stores = [], [], [], []
    for c in range(chunks):
        span = pl.ds(c * CHUNK, CHUNK)
        k_loads.append(pltpu.make_async_copy(ck_hbm.at[span], nk_ref.at[span], sem_k.at[c]))
        v_loads.append(pltpu.make_async_copy(cv_hbm.at[span], nv_ref.at[span], sem_v.at[c]))
        k_stores.append(pltpu.make_async_copy(nk_ref.at[span], nk_hbm.at[span], sem_ko.at[c]))
        v_stores.append(pltpu.make_async_copy(nv_ref.at[span], nv_hbm.at[span], sem_vo.at[c]))
        k_loads[c].start()
        v_loads[c].start()

    sub = lax.broadcasted_iota(jnp.int32, (8, 128), 0)
    for g in range(rows // 8):
        acc = jnp.zeros((8, 128), jnp.int32)
        for r in range(8):
            acc = jnp.where(sub == r, pos_ref[8 * g + r], acc)
        posm[pl.ds(8 * g, 8), :] = acc
    angles = posm[...].astype(F32) * freq_ref[...]
    cos = jnp.cos(angles)
    sin = jnp.sin(angles)

    loads[0].wait()
    loads[1].wait()
    wide = tok[...].astype(F32)
    inv_rms = lax.rsqrt(jnp.mean(wide * wide, axis=-1, keepdims=True) + NORM_EPS)
    normed = (wide * inv_rms * gain[...].astype(F32).reshape(1, -1)).astype(BF16)

    def rope(lin):
        a, b = lin[:, :half], lin[:, half:]
        return jnp.concatenate([a * cos - b * sin, b * cos + a * sin], axis=-1)

    loads[2].wait()
    knew[...] = rope(jnp.dot(normed, wk[...], preferred_element_type=F32)).astype(BF16).astype(F32)
    loads[3].wait()
    vnew[...] = jnp.dot(normed, wv[...], preferred_element_type=F32).astype(BF16).astype(F32)
    loads[4].wait()
    heads = wq.shape[1] // dim
    q_lin = jnp.dot(normed, wq[...], preferred_element_type=F32)
    q_rot = [rope(q_lin[:, h * dim:(h + 1) * dim]) for h in range(heads)]
    for g in range(rows // 8):
        qs[g] = jnp.concatenate([q_rot[h][8 * g:8 * g + 8] for h in range(heads)], axis=0).astype(BF16)

    sub16 = lax.broadcasted_iota(jnp.int32, (16, dim), 0)
    lane = lax.broadcasted_iota(jnp.int32, (16, local_slots), 1) + base
    lane128 = lax.broadcasted_iota(jnp.int32, (16, 128), 1)

    def patch(ref, new_ref, b, offset):
        inside = jnp.clip(offset, 0, local_slots - 1)
        start = pl.multiple_of((inside // 16) * 16, 16)
        old = ref[b, pl.ds(start, 16), :].astype(F32)
        ref[b, pl.ds(start, 16), :] = jnp.where(sub16 == offset - start, new_ref[pl.ds(b, 1), :], old).astype(BF16)

    for c in range(chunks):
        offsets = [jnp.bitwise_and(pos_ref[c * CHUNK + j], slots - 1) - base for j in range(CHUNK)]
        k_loads[c].wait()
        for j in range(CHUNK):
            patch(nk_ref, knew, c * CHUNK + j, offsets[j])
        k_stores[c].start()
        probs = []
        for g in range(c * CHUNK // 8, (c + 1) * CHUNK // 8):
            query = qs[g]
            scores = jnp.zeros((16, local_slots), F32)
            for j in range(8):
                one = lax.dot_general(query, nk_ref[8 * g + j], (((1,), (1,)), ((), ())), preferred_element_type=F32)
                scores = jnp.where(jnp.bitwise_and(sub16, 7) == j, one, scores)
            scores = scores * (1.0 / math.sqrt(dim))
            pos8 = posm[pl.ds(8 * g, 8), :]
            pos16 = jnp.concatenate([pos8, pos8], axis=0)
            limit = jnp.where(pos16 >= slots - 1, slots, pos16)
            valid = lane <= jnp.concatenate([limit] * (local_slots // 128), axis=1)
            top = jnp.max(jnp.where(valid, scores, -jnp.inf), axis=-1, keepdims=True)
            safe = jnp.where(top == -jnp.inf, 0.0, top)
            weights = jnp.exp(jnp.where(valid, scores - safe, -jnp.inf))
            total = jnp.sum(weights, axis=-1, keepdims=True)
            probs.append((g, weights.astype(BF16), top, total))
        v_loads[c].wait()
        for j in range(CHUNK):
            patch(nv_ref, vnew, c * CHUNK + j, offsets[j])
        v_stores[c].start()
        for g, weights, top, total in probs:
            out = jnp.zeros((16, dim), F32)
            for j in range(8):
                one = jnp.dot(weights, nv_ref[8 * g + j], preferred_element_type=F32)
                out = jnp.where(jnp.bitwise_and(sub16, 7) == j, one, out)
            stats = jnp.where(lane128 < 64, top, total)
            dest, upper = g // 2, g % 2
            for h in range(heads):
                span = pl.ds(16 * h + 8 * upper, 8)
                part_ref[dest, span, 0:dim] = out[8 * h:8 * h + 8]
                part_ref[dest, span, dim:dim + 128] = stats[8 * h:8 * h + 8]
    for copy in k_stores + v_stores:
        copy.wait()


def attend(tokens, positions, cache_k, cache_v, gain, w_q, w_k, w_v, sp_size):
    rows, width = tokens.shape
    _, local_slots, _, dim = cache_k.shape
    heads = w_q.shape[1] // dim
    freq = (ROPE_THETA ** (-2.0 * np.arange(dim // 2, dtype=np.float64) / dim)).astype(np.float32)
    ck = cache_k.reshape(rows, local_slots, dim)
    cv = cache_v.reshape(rows, local_slots, dim)
    any_spec = pl.BlockSpec(memory_space=pltpu.HBM)
    vmem_spec = pl.BlockSpec(memory_space=pltpu.VMEM)
    chunks = rows // CHUNK
    nk, nv, part = pl.pallas_call(
        functools.partial(attn_kernel, sp_size),
        name="attend",
        out_shape=(
            jax.ShapeDtypeStruct((rows, local_slots, dim), BF16),
            jax.ShapeDtypeStruct((rows, local_slots, dim), BF16),
            jax.ShapeDtypeStruct((sp_size, heads * rows // sp_size, dim + 128), F32),
        ),
        in_specs=[pl.BlockSpec(memory_space=pltpu.SMEM), vmem_spec] + [any_spec] * 7,
        out_specs=[any_spec, any_spec, vmem_spec],
        scratch_shapes=[
            pltpu.VMEM((rows, local_slots, dim), BF16),
            pltpu.VMEM((rows, local_slots, dim), BF16),
            pltpu.VMEM((rows, width), BF16),
            pltpu.VMEM((width,), BF16),
            pltpu.VMEM(w_q.shape, BF16),
            pltpu.VMEM(w_k.shape, BF16),
            pltpu.VMEM(w_v.shape, BF16),
            pltpu.VMEM((rows // 8, 8 * heads, dim), BF16),
            pltpu.VMEM((rows, dim), F32),
            pltpu.VMEM((rows, dim), F32),
            pltpu.VMEM((rows, 128), jnp.int32),
            pltpu.SemaphoreType.DMA((5,)),
            pltpu.SemaphoreType.DMA((chunks,)),
            pltpu.SemaphoreType.DMA((chunks,)),
            pltpu.SemaphoreType.DMA((chunks,)),
            pltpu.SemaphoreType.DMA((chunks,)),
        ],
        compiler_params=pltpu.CompilerParams(vmem_limit_bytes=VMEM_A),
        cost_estimate=pl.CostEstimate(flops=2 * rows * width * 1024, bytes_accessed=22 << 20, transcendentals=0),
    )(positions, jnp.asarray(freq).reshape(1, -1), tokens, gain, w_q, w_k, w_v, ck, cv)
    return nk.reshape(cache_k.shape), nv.reshape(cache_v.shape), part


VMEM_A = 67043328 - (448 << 10)


def solution(mesh):
    sp_size = mesh.shape["sp"]
    cache_spec = P("dp", "sp", "tp", None)
    row_spec = P("dp", None)
    col_spec = P(None, "tp")
    in_specs = (row_spec, P("dp"), cache_spec, cache_spec, P(None), col_spec, col_spec, col_spec, P("tp", None), P(None), col_spec, col_spec, P("tp", None))
    out_specs = (row_spec, cache_spec, cache_spec)

    def local_step(tokens, positions, cache_k, cache_v, attn_gain, w_q, w_k, w_v, w_o, mlp_gain, w_gate, w_up, w_down):
        rows = tokens.shape[0]
        dim = cache_k.shape[3]
        new_k, new_v, part = attend(tokens, positions, cache_k, cache_v, attn_gain, w_q, w_k, w_v, sp_size)
        o = part[:, :, :dim]; m = part[:, :, dim:dim + 1]; l = part[:, :, dim + 64:dim + 65]
        gm = lax.pmax(m, "sp")
        f = jnp.exp(m - gm)
        tot = lax.psum(jnp.concatenate([o * f, l * f], axis=-1), "sp")
        att = (tot[..., :dim] / tot[..., dim:]).astype(BF16)
        att = att.reshape(4, 2, 16, dim).transpose(0, 2, 1, 3).reshape(rows, 2 * dim)
        attn_proj = lax.psum(jnp.dot(att, w_o, preferred_element_type=F32), "tp")
        hidden = (tokens.astype(F32) + attn_proj).astype(BF16)
        normed_mlp = rms_norm(hidden, mlp_gain)
        gate_proj = jnp.dot(normed_mlp, w_gate, preferred_element_type=F32)
        up_proj = jnp.dot(normed_mlp, w_up, preferred_element_type=F32)
        activated = (jax.nn.silu(gate_proj) * up_proj).astype(BF16)
        mlp_down = lax.psum(jnp.dot(activated, w_down, preferred_element_type=F32), "tp")
        layer_out = (hidden.astype(F32) + mlp_down).astype(BF16)
        return layer_out, new_k, new_v

    return jax.shard_map(local_step, mesh=mesh, in_specs=in_specs, out_specs=out_specs, check_vma=False)
```

```python
import functools
import math

import jax
import jax.numpy as jnp
import numpy as np
from jax import lax
from jax.experimental import pallas as pl
from jax.experimental.pallas import tpu as pltpu
from jax.sharding import PartitionSpec as P

NORM_EPS = 1e-5
ROPE_THETA = 10000.0
F32 = jnp.float32
BF16 = jnp.bfloat16
CHUNK = 16


def attn_kernel(sp_size, pos_ref, freq_ref, tok_hbm, gain_hbm, wq_hbm, wk_hbm, wv_hbm, ck_hbm, cv_hbm,
                nk_hbm, nv_hbm, part_ref, nk_ref, nv_ref, tok, gain, wq, wk, wv, qs, knew, vnew, posm,
                sem_w, sem_k, sem_v, sem_ko, sem_vo):
    rows = tok.shape[0]
    local_slots = nk_ref.shape[1]
    dim = nk_ref.shape[2]
    half = dim // 2
    slots = local_slots * sp_size
    chunks = rows // CHUNK
    base = lax.axis_index("sp") * local_slots

    loads = [pltpu.make_async_copy(src, dst, sem_w.at[i]) for i, (src, dst) in enumerate(
        ((tok_hbm, tok), (gain_hbm, gain), (wk_hbm, wk), (wv_hbm, wv), (wq_hbm, wq)))]
    for copy in loads:
        copy.start()
    k_loads, v_loads, k_stores, v_stores = [], [], [], []
    for c in range(chunks):
        span = pl.ds(c * CHUNK, CHUNK)
        k_loads.append(pltpu.make_async_copy(ck_hbm.at[span], nk_ref.at[span], sem_k.at[c]))
        v_loads.append(pltpu.make_async_copy(cv_hbm.at[span], nv_ref.at[span], sem_v.at[c]))
        k_stores.append(pltpu.make_async_copy(nk_ref.at[span], nk_hbm.at[span], sem_ko.at[c]))
        v_stores.append(pltpu.make_async_copy(nv_ref.at[span], nv_hbm.at[span], sem_vo.at[c]))
        k_loads[c].start()
        v_loads[c].start()

    sub = lax.broadcasted_iota(jnp.int32, (8, 128), 0)
    for g in range(rows // 8):
        acc = jnp.zeros((8, 128), jnp.int32)
        for r in range(8):
            acc = jnp.where(sub == r, pos_ref[8 * g + r], acc)
        posm[pl.ds(8 * g, 8), :] = acc
    angles = posm[...].astype(F32) * freq_ref[...]
    cos = jnp.cos(angles)
    sin = jnp.sin(angles)

    loads[0].wait()
    loads[1].wait()
    wide = tok[...].astype(F32)
    inv_rms = lax.rsqrt(jnp.mean(wide * wide, axis=-1, keepdims=True) + NORM_EPS)
    normed = (wide * inv_rms * gain[...].astype(F32).reshape(1, -1)).astype(BF16)

    def rope(lin):
        a, b = lin[:, :half], lin[:, half:]
        return jnp.concatenate([a * cos - b * sin, b * cos + a * sin], axis=-1)

    loads[2].wait()
    knew[...] = rope(jnp.dot(normed, wk[...], preferred_element_type=F32)).astype(BF16).astype(F32)
    loads[3].wait()
    vnew[...] = jnp.dot(normed, wv[...], preferred_element_type=F32).astype(BF16).astype(F32)
    loads[4].wait()
    heads = wq.shape[1] // dim
    q_lin = jnp.dot(normed, wq[...], preferred_element_type=F32)
    q_rot = [rope(q_lin[:, h * dim:(h + 1) * dim]) for h in range(heads)]
    for g in range(rows // 8):
        qs[g] = jnp.concatenate([q_rot[h][8 * g:8 * g + 8] for h in range(heads)], axis=0).astype(BF16)

    sub16 = lax.broadcasted_iota(jnp.int32, (16, dim), 0)
    lane = lax.broadcasted_iota(jnp.int32, (16, local_slots), 1) + base
    lane128 = lax.broadcasted_iota(jnp.int32, (16, 128), 1)

    def patch(ref, new_ref, b, offset):
        inside = jnp.clip(offset, 0, local_slots - 1)
        start = pl.multiple_of((inside // 16) * 16, 16)
        old = ref[b, pl.ds(start, 16), :].astype(F32)
        ref[b, pl.ds(start, 16), :] = jnp.where(sub16 == offset - start, new_ref[pl.ds(b, 1), :], old).astype(BF16)

    for c in range(chunks):
        offsets = [jnp.bitwise_and(pos_ref[c * CHUNK + j], slots - 1) - base for j in range(CHUNK)]
        k_loads[c].wait()
        for j in range(CHUNK):
            patch(nk_ref, knew, c * CHUNK + j, offsets[j])
        k_stores[c].start()
        probs = []
        for g in range(c * CHUNK // 8, (c + 1) * CHUNK // 8):
            query = qs[g]
            scores = jnp.zeros((16, local_slots), F32)
            for j in range(8):
                one = lax.dot_general(query, nk_ref[8 * g + j], (((1,), (1,)), ((), ())), preferred_element_type=F32)
                scores = jnp.where(jnp.bitwise_and(sub16, 7) == j, one, scores)
            scores = scores * (1.0 / math.sqrt(dim))
            pos8 = posm[pl.ds(8 * g, 8), :]
            pos16 = jnp.concatenate([pos8, pos8], axis=0)
            limit = jnp.where(pos16 >= slots - 1, slots, pos16)
            valid = lane <= jnp.concatenate([limit] * (local_slots // 128), axis=1)
            top = jnp.max(jnp.where(valid, scores, -jnp.inf), axis=-1, keepdims=True)
            safe = jnp.where(top == -jnp.inf, 0.0, top)
            weights = jnp.exp(jnp.where(valid, scores - safe, -jnp.inf))
            total = jnp.sum(weights, axis=-1, keepdims=True)
            probs.append((g, weights.astype(BF16), top, total))
        v_loads[c].wait()
        for j in range(CHUNK):
            patch(nv_ref, vnew, c * CHUNK + j, offsets[j])
        v_stores[c].start()
        for g, weights, top, total in probs:
            out = jnp.zeros((16, dim), F32)
            for j in range(8):
                one = jnp.dot(weights, nv_ref[8 * g + j], preferred_element_type=F32)
                out = jnp.where(jnp.bitwise_and(sub16, 7) == j, one, out)
            stats = jnp.where(lane128 < 64, top, total)
            dest, upper = g // 2, g % 2
            for h in range(heads):
                span = pl.ds(16 * h + 8 * upper, 8)
                part_ref[dest, span, 0:dim] = out[8 * h:8 * h + 8]
                part_ref[dest, span, dim:dim + 128] = stats[8 * h:8 * h + 8]
    for copy in k_stores + v_stores:
        copy.wait()


def attend(tokens, positions, cache_k, cache_v, gain, w_q, w_k, w_v, sp_size):
    rows, width = tokens.shape
    _, local_slots, _, dim = cache_k.shape
    heads = w_q.shape[1] // dim
    freq = (ROPE_THETA ** (-2.0 * np.arange(dim // 2, dtype=np.float64) / dim)).astype(np.float32)
    ck = cache_k.reshape(rows, local_slots, dim)
    cv = cache_v.reshape(rows, local_slots, dim)
    any_spec = pl.BlockSpec(memory_space=pltpu.HBM)
    vmem_spec = pl.BlockSpec(memory_space=pltpu.VMEM)
    chunks = rows // CHUNK
    nk, nv, part = pl.pallas_call(
        functools.partial(attn_kernel, sp_size),
        name="attend",
        out_shape=(
            jax.ShapeDtypeStruct((rows, local_slots, dim), BF16),
            jax.ShapeDtypeStruct((rows, local_slots, dim), BF16),
            jax.ShapeDtypeStruct((sp_size, heads * rows // sp_size, dim + 128), F32),
        ),
        in_specs=[pl.BlockSpec(memory_space=pltpu.SMEM), vmem_spec] + [any_spec] * 7,
        out_specs=[any_spec, any_spec, vmem_spec],
        scratch_shapes=[
            pltpu.VMEM((rows, local_slots, dim), BF16),
            pltpu.VMEM((rows, local_slots, dim), BF16),
            pltpu.VMEM((rows, width), BF16),
            pltpu.VMEM((width,), BF16),
            pltpu.VMEM(w_q.shape, BF16),
            pltpu.VMEM(w_k.shape, BF16),
            pltpu.VMEM(w_v.shape, BF16),
            pltpu.VMEM((rows // 8, 8 * heads, dim), BF16),
            pltpu.VMEM((rows, dim), F32),
            pltpu.VMEM((rows, dim), F32),
            pltpu.VMEM((rows, 128), jnp.int32),
            pltpu.SemaphoreType.DMA((5,)),
            pltpu.SemaphoreType.DMA((chunks,)),
            pltpu.SemaphoreType.DMA((chunks,)),
            pltpu.SemaphoreType.DMA((chunks,)),
            pltpu.SemaphoreType.DMA((chunks,)),
        ],
        compiler_params=pltpu.CompilerParams(vmem_limit_bytes=VMEM_A),
        cost_estimate=pl.CostEstimate(flops=2 * rows * width * 1024, bytes_accessed=22 << 20, transcendentals=0),
    )(positions, jnp.asarray(freq).reshape(1, -1), tokens, gain, w_q, w_k, w_v, ck, cv)
    return nk.reshape(cache_k.shape), nv.reshape(cache_v.shape), part


VMEM_A = 67043328 - (448 << 10)


def partner(index, k):
    if k == 0:
        return index
    if k == 1:
        return index + 1 - 2 * lax.rem(index, 2)
    if k == 2:
        return lax.rem(index + 2, 4)
    return 3 - index


def finish_kernel(part_ref, tok_hbm, gain_hbm, wo_hbm, wg_hbm, wu_hbm, wd_hbm, out_ref,
                  wo, wg, wu, wd, tokv, gain, r1, y2, r2, r3, y4, r4, fin,
                  sem_w, s1, g1, s2, g2, s3, g3, s4, g4, s5z, g5z, s5y, g5y, s5c, g5c):
    s = lax.axis_index("sp")
    z = lax.axis_index("tp")
    width = wo.shape[1]
    wide = width // 2
    dim = part_ref.shape[2] - 128
    own_rows = part_ref.shape[1] // 2

    loads = [pltpu.make_async_copy(src, dst, sem_w.at[i]) for i, (src, dst) in enumerate((
        (tok_hbm.at[pl.ds(pl.multiple_of(s * own_rows, own_rows), own_rows)], tokv), (gain_hbm, gain),
        (wo_hbm, wo), (wg_hbm, wg), (wu_hbm, wu), (wd_hbm, wd)))]
    for copy in loads:
        copy.start()

    barrier = pltpu.get_barrier_semaphore()
    for k in (1, 2, 3):
        pl.semaphore_signal(barrier, inc=1, device_id={"tp": partner(z, k)}, device_id_type=MESH)
        pl.semaphore_signal(barrier, inc=1, device_id={"sp": partner(s, k)}, device_id_type=MESH)
    pl.semaphore_wait(barrier, 6)

    def send(src, dst, send_sem, recv_sem, **target):
        copy = pltpu.make_async_remote_copy(src_ref=src, dst_ref=dst, send_sem=send_sem, recv_sem=recv_sem,
                                            device_id=target, device_id_type=MESH)
        copy.start()
        return copy

    first = [send(part_ref.at[partner(s, k)], r1.at[k - 1], s1.at[k - 1], g1.at[k - 1], sp=partner(s, k)) for k in (3, 2, 1)]

    sub = lax.broadcasted_iota(jnp.int32, (8, wide), 0)
    low = sub < 4

    def piece(left, right, d):
        t = d // 2
        a, b = left[8 * t:8 * t + 8], right[8 * t:8 * t + 8]
        mask = low[:, :a.shape[1]]
        return jnp.where(mask, a, b) if d % 2 == 0 else jnp.where(mask, b, a)

    def swap(x):
        return jnp.concatenate([pltpu.roll(x[8 * t:8 * t + 8], 4, 0) for t in range(x.shape[0] // 8)], axis=0)

    def rows_of(four):
        lefts, rights = [], []
        for t in range(2):
            a, b = four[2 * t], four[2 * t + 1]
            mask = low[:, :a.shape[1]]
            lefts.append(jnp.where(mask, a, b))
            rights.append(pltpu.roll(jnp.where(mask, b, a), 4, 0))
        return jnp.concatenate(lefts, axis=0), jnp.concatenate(rights, axis=0)

    loads[0].wait()
    loads[1].wait()
    tok = tokv[...].astype(F32)
    tok_l, tok_r = tok[:, :wide], swap(tok[:, wide:])
    tok_piece = piece(tok_l, tok_r, 0)
    for d in (1, 2, 3):
        tok_piece = jnp.where(z == d, piece(tok_l, tok_r, d), tok_piece)
    gain_row = gain[...].astype(F32).reshape(1, -1)
    even = lax.rem(z, 2) == 0
    gain_piece = jnp.where(jnp.where(even, sub, 7 - sub) < 4, gain_row[:, :wide], gain_row[:, wide:])

    for copy in first:
        copy.wait_recv()
    parts = [part_ref[s], r1[0], r1[1], r1[2]]
    tops = [p[:, dim:dim + 1] for p in parts]
    sums = [p[:, dim + 64:dim + 65] for p in parts]
    top = jnp.maximum(jnp.maximum(tops[0], tops[1]), jnp.maximum(tops[2], tops[3]))
    scales = [jnp.exp(t - top) for t in tops]
    total = sum(f * l for f, l in zip(scales, sums))
    mixed = sum(f * p[:, :dim] for f, p in zip(scales, parts)) / total
    att = jnp.concatenate([mixed[:own_rows], mixed[own_rows:]], axis=1)
    att_swapped = swap(att).astype(BF16)
    att = att.astype(BF16)

    loads[2].wait()
    second = []
    for c, (at, size) in enumerate(CUT_O):
        left = jnp.dot(att, wo[:, at:at + size], preferred_element_type=F32)
        right = jnp.dot(att_swapped, wo[:, wide + at:wide + at + size], preferred_element_type=F32)
        for d in range(4):
            y2[d, :, at:at + size] = piece(left, right, d)
        for k in (3, 2, 1):
            second.append(send(y2.at[partner(z, k), :, pl.ds(at, size)], r2.at[k - 1, :, pl.ds(at, size)],
                               s2.at[k - 1, c], g2.at[k - 1, c], tp=partner(z, k)))
    for copy in second:
        copy.wait_recv()
    hidden = (tok_piece + (y2[z] + r2[0] + r2[1] + r2[2])).astype(BF16).astype(F32)
    squares = jnp.sum(hidden * hidden, axis=-1, keepdims=True)
    squares = jnp.broadcast_to(squares, (8, 128))
    squares = squares + pltpu.roll(squares, 4, 0)
    inv_rms = lax.rsqrt(squares[:, :1] / width + NORM_EPS)
    r3[z] = (hidden * inv_rms * gain_piece).astype(BF16).astype(F32)

    third = []
    for c, (at, size) in enumerate(CUT_M):
        for k in (3, 2, 1):
            third.append(send(r3.at[z, :, pl.ds(at, size)], r3.at[z, :, pl.ds(at, size)], s3.at[k - 1, c], g3.at[k - 1, c],
                              tp=partner(z, k)))
    loads[3].wait()
    loads[4].wait()
    gate = up = None
    for c, (at, size) in enumerate(CUT_M):
        for copy in third[3 * c:3 * c + 3]:
            copy.wait_recv()
        left, right = rows_of([r3[d, :, at:at + size] for d in range(4)])
        left, right = left.astype(BF16), right.astype(BF16)
        pair = []
        for w in (wg, wu):
            pair.append(jnp.dot(left, w[at:at + size, :], preferred_element_type=F32)
                        + jnp.dot(right, w[wide + at:wide + at + size, :], preferred_element_type=F32))
        gate = pair[0] if gate is None else gate + pair[0]
        up = pair[1] if up is None else up + pair[1]
    act = gate * (1.0 / (1.0 + jnp.exp(-gate))) * up
    act = act.astype(BF16)
    act_swapped = swap(act.astype(F32)).astype(BF16)

    loads[5].wait()
    fourth = []
    for c, (at, size) in enumerate(CUT_D):
        left = jnp.dot(act, wd[:, at:at + size], preferred_element_type=F32)
        right = jnp.dot(act_swapped, wd[:, wide + at:wide + at + size], preferred_element_type=F32)
        for d in range(4):
            y4[d, :, at:at + size] = piece(left, right, d)
        for k in (3, 2, 1):
            fourth.append(send(y4.at[partner(z, k), :, pl.ds(at, size)], r4.at[k - 1, :, pl.ds(at, size)],
                               s4.at[k - 1, c], g4.at[k - 1, c], tp=partner(z, k)))

    along, across, beside = {}, {}, {}
    for c, (at, size) in enumerate(CUT_D):
        for copy in fourth[3 * c:3 * c + 3]:
            copy.wait_recv()
        span = pl.ds(at, size)
        total = y4[z, :, at:at + size] + r4[0, :, at:at + size] + r4[1, :, at:at + size] + r4[2, :, at:at + size]
        fin[s, z, :, at:at + size] = (hidden[:, at:at + size] + total).astype(BF16).astype(F32)
        mine = fin.at[s, z, :, span]
        for k in (3, 2, 1):
            along[c, k] = send(mine, mine, s5z.at[k - 1, c], g5z.at[k - 1, c], tp=partner(z, k))
        across[c, 0] = send(mine, mine, s5y.at[0, c], g5y.at[0, c], sp=partner(s, 2))
        beside[c, 0] = send(mine, mine, s5c.at[0, c], g5c.at[0, c], sp=partner(s, 1))
    for c, (at, size) in enumerate(CUT_D):
        span = pl.ds(at, size)
        for k in range(4):
            if k:
                along[c, k].wait_recv()
                came = fin.at[s, partner(z, k), :, span]
                across[c, k] = send(came, came, s5y.at[k, c], g5y.at[k, c], sp=partner(s, 2))
                beside[c, k] = send(came, came, s5c.at[k, c], g5c.at[k, c], sp=partner(s, 1))
        for k in range(4):
            across[c, k].wait_recv()
            came = fin.at[partner(s, 2), partner(z, k), :, span]
            beside[c, 4 + k] = send(came, came, s5c.at[4 + k, c], g5c.at[4 + k, c], sp=partner(s, 1))
    for copy in beside.values():
        copy.wait_recv()
    for r in range(4):
        left, right = rows_of([fin[r, d] for d in range(4)])
        out_ref[pl.ds(own_rows * r, own_rows), 0:wide] = left.astype(BF16)
        out_ref[pl.ds(own_rows * r, own_rows), wide:width] = right.astype(BF16)
    for copy in first + second + third + fourth + list(along.values()) + list(across.values()) + list(beside.values()):
        copy.wait_send()


MESH = pl.DeviceIdType.MESH
CUT_O = ((0, 512), (512, 768))
CUT_M = ((0, 768), (768, 512))
CUT_D = ((0, 512), (512, 768))


def finish(part, tokens, gain, w_o, w_gate, w_up, w_down):
    rows, width = tokens.shape
    hbm = pl.BlockSpec(memory_space=pltpu.HBM)
    vmem = pl.BlockSpec(memory_space=pltpu.VMEM)
    own = part.shape[1] // 2
    half = width // 2
    dma = pltpu.SemaphoreType.DMA
    return pl.pallas_call(
        finish_kernel,
        name="finish",
        out_shape=jax.ShapeDtypeStruct((rows, width), BF16),
        in_specs=[vmem] + [hbm] * 6,
        out_specs=vmem,
        scratch_shapes=[
            pltpu.VMEM(w_o.shape, BF16),
            pltpu.VMEM(w_gate.shape, BF16),
            pltpu.VMEM(w_up.shape, BF16),
            pltpu.VMEM(w_down.shape, BF16),
            pltpu.VMEM((own, width), BF16),
            pltpu.VMEM((width,), BF16),
            pltpu.VMEM((3,) + part.shape[1:], F32),
            pltpu.VMEM((4, 8, half), F32),
            pltpu.VMEM((3, 8, half), F32),
            pltpu.VMEM((4, 8, half), F32),
            pltpu.VMEM((4, 8, half), F32),
            pltpu.VMEM((3, 8, half), F32),
            pltpu.VMEM((4, 4, 8, half), F32),
            dma((6,)),
            dma((3,)), dma((3,)),
            dma((3, len(CUT_O))), dma((3, len(CUT_O))),
            dma((3, len(CUT_M))), dma((3, len(CUT_M))),
            dma((3, len(CUT_D))), dma((3, len(CUT_D))),
            dma((3, len(CUT_D))), dma((3, len(CUT_D))),
            dma((4, len(CUT_D))), dma((4, len(CUT_D))),
            dma((8, len(CUT_D))), dma((8, len(CUT_D))),
        ],
        compiler_params=pltpu.CompilerParams(collective_id=0, has_side_effects=True, vmem_limit_bytes=VMEM_B),
        cost_estimate=pl.CostEstimate(flops=2 * 16 * width * 2560 * 3, bytes_accessed=42 << 20, transcendentals=0),
    )(part, tokens, gain, w_o, w_gate, w_up, w_down)


VMEM_B = 62 << 20


def solution(mesh):
    sp_size = mesh.shape["sp"]
    cache_spec = P("dp", "sp", "tp", None)
    row_spec = P("dp", None)
    col_spec = P(None, "tp")
    in_specs = (row_spec, P("dp"), cache_spec, cache_spec, P(None), col_spec, col_spec, col_spec, P("tp", None), P(None), col_spec, col_spec, P("tp", None))
    out_specs = (row_spec, cache_spec, cache_spec)

    def local_step(tokens, positions, cache_k, cache_v, attn_gain, w_q, w_k, w_v, w_o, mlp_gain, w_gate, w_up, w_down):
        new_k, new_v, part = attend(tokens, positions, cache_k, cache_v, attn_gain, w_q, w_k, w_v, sp_size)
        layer_out = finish(part, tokens, mlp_gain, w_o, w_gate, w_up, w_down)
        return layer_out, new_k, new_v

    return jax.shard_map(local_step, mesh=mesh, in_specs=in_specs, out_specs=out_specs, check_vma=False)
```

```python
import functools
import math

import jax
import jax.numpy as jnp
import numpy as np
from jax import lax
from jax.experimental import pallas as pl
from jax.experimental.pallas import tpu as pltpu
from jax.sharding import PartitionSpec as P

NORM_EPS = 1e-5
ROPE_THETA = 10000.0
F32 = jnp.float32
BF16 = jnp.bfloat16
CHUNK = 16


def attn_kernel(sp_size, pos_hbm, freq_hbm, tok_hbm, gain_hbm, wq_hbm, wk_hbm, wv_hbm, ck_hbm, cv_hbm,
                nk_hbm, nv_hbm, part_ref, pos_ref, freq_ref, nk_ref, nv_ref, tok, gain, wq, wk, wv, qs, knew, vnew, posm,
                sem_w, sem_k, sem_v, sem_ko, sem_vo):
    rows = tok.shape[0]
    local_slots = nk_ref.shape[1]
    dim = nk_ref.shape[2]
    half = dim // 2
    slots = local_slots * sp_size
    chunks = rows // CHUNK
    base = lax.axis_index("sp") * local_slots

    loads = [pltpu.make_async_copy(src, dst, sem_w.at[i]) for i, (src, dst) in enumerate(
        ((tok_hbm, tok), (gain_hbm, gain), (wk_hbm, wk), (wv_hbm, wv), (wq_hbm, wq), (pos_hbm, pos_ref), (freq_hbm, freq_ref)))]
    for i in (5, 6, 0, 1, 2, 3, 4):
        loads[i].start()
    k_loads, v_loads, k_stores, v_stores = [], [], [], []
    for c in range(chunks):
        span = pl.ds(c * CHUNK, CHUNK)
        k_loads.append(pltpu.make_async_copy(ck_hbm.at[span], nk_ref.at[span], sem_k.at[c]))
        v_loads.append(pltpu.make_async_copy(cv_hbm.at[span], nv_ref.at[span], sem_v.at[c]))
        k_stores.append(pltpu.make_async_copy(nk_ref.at[span], nk_hbm.at[span], sem_ko.at[c]))
        v_stores.append(pltpu.make_async_copy(nv_ref.at[span], nv_hbm.at[span], sem_vo.at[c]))

    loads[5].wait()
    loads[6].wait()
    sub = lax.broadcasted_iota(jnp.int32, (8, 128), 0)
    for g in range(rows // 8):
        acc = jnp.zeros((8, 128), jnp.int32)
        for r in range(8):
            acc = jnp.where(sub == r, pos_ref[8 * g + r], acc)
        posm[pl.ds(8 * g, 8), :] = acc
    angles = posm[...].astype(F32) * freq_ref[...]
    cos = jnp.cos(angles)
    sin = jnp.sin(angles)

    loads[0].wait()
    loads[1].wait()
    wide = tok[...].astype(F32)
    inv_rms = lax.rsqrt(jnp.mean(wide * wide, axis=-1, keepdims=True) + NORM_EPS)
    normed = (wide * inv_rms * gain[...].astype(F32).reshape(1, -1)).astype(BF16)

    def fetch(c):
        if c < chunks:
            k_loads[c].start()
            v_loads[c].start()

    def rope(lin):
        a, b = lin[:, :half], lin[:, half:]
        return jnp.concatenate([a * cos - b * sin, b * cos + a * sin], axis=-1)

    loads[2].wait()
    fetch(0)
    knew[...] = rope(jnp.dot(normed, wk[...], preferred_element_type=F32)).astype(BF16).astype(F32)
    loads[3].wait()
    vnew[...] = jnp.dot(normed, wv[...], preferred_element_type=F32).astype(BF16).astype(F32)
    loads[4].wait()
    fetch(1)
    heads = wq.shape[1] // dim
    q_lin = jnp.dot(normed, wq[...], preferred_element_type=F32)
    q_rot = [rope(q_lin[:, h * dim:(h + 1) * dim]) for h in range(heads)]
    for g in range(rows // 8):
        qs[g] = jnp.concatenate([q_rot[h][8 * g:8 * g + 8] for h in range(heads)], axis=0).astype(BF16)

    sub16 = lax.broadcasted_iota(jnp.int32, (16, dim), 0)
    lane = lax.broadcasted_iota(jnp.int32, (16, local_slots), 1) + base
    lane128 = lax.broadcasted_iota(jnp.int32, (16, 128), 1)

    def patch(ref, new_ref, b, offset):
        inside = jnp.clip(offset, 0, local_slots - 1)
        start = pl.multiple_of((inside // 16) * 16, 16)
        old = ref[b, pl.ds(start, 16), :].astype(F32)
        ref[b, pl.ds(start, 16), :] = jnp.where(sub16 == offset - start, new_ref[pl.ds(b, 1), :], old).astype(BF16)

    for c in range(chunks):
        offsets = [jnp.bitwise_and(pos_ref[c * CHUNK + j], slots - 1) - base for j in range(CHUNK)]
        k_loads[c].wait()
        fetch(c + 2)
        for j in range(CHUNK):
            patch(nk_ref, knew, c * CHUNK + j, offsets[j])
        k_stores[c].start()
        probs = []
        for g in range(c * CHUNK // 8, (c + 1) * CHUNK // 8):
            query = qs[g]
            scores = jnp.zeros((16, local_slots), F32)
            for j in range(8):
                one = lax.dot_general(query, nk_ref[8 * g + j], (((1,), (1,)), ((), ())), preferred_element_type=F32)
                scores = jnp.where(jnp.bitwise_and(sub16, 7) == j, one, scores)
            scores = scores * (1.0 / math.sqrt(dim))
            pos8 = posm[pl.ds(8 * g, 8), :]
            pos16 = jnp.concatenate([pos8, pos8], axis=0)
            limit = jnp.where(pos16 >= slots - 1, slots, pos16)
            valid = lane <= jnp.concatenate([limit] * (local_slots // 128), axis=1)
            top = jnp.max(jnp.where(valid, scores, -jnp.inf), axis=-1, keepdims=True)
            safe = jnp.where(top == -jnp.inf, 0.0, top)
            weights = jnp.exp(jnp.where(valid, scores - safe, -jnp.inf))
            total = jnp.sum(weights, axis=-1, keepdims=True)
            probs.append((g, weights.astype(BF16), top, total))
        v_loads[c].wait()
        for j in range(CHUNK):
            patch(nv_ref, vnew, c * CHUNK + j, offsets[j])
        v_stores[c].start()
        for g, weights, top, total in probs:
            out = jnp.zeros((16, dim), F32)
            for j in range(8):
                one = jnp.dot(weights, nv_ref[8 * g + j], preferred_element_type=F32)
                out = jnp.where(jnp.bitwise_and(sub16, 7) == j, one, out)
            stats = jnp.where(lane128 < 64, top, total)
            dest, upper = g // 2, g % 2
            for h in range(heads):
                span = pl.ds(16 * h + 8 * upper, 8)
                part_ref[dest, span, 0:dim] = out[8 * h:8 * h + 8]
                part_ref[dest, span, dim:dim + 128] = stats[8 * h:8 * h + 8]
    for copy in k_stores + v_stores:
        copy.wait()


def in_hbm(*arrays):
    return [pltpu.with_memory_space_constraint(x, pltpu.HBM) for x in arrays]


def attend(tokens, positions, cache_k, cache_v, gain, w_q, w_k, w_v, sp_size):
    rows, width = tokens.shape
    _, local_slots, _, dim = cache_k.shape
    heads = w_q.shape[1] // dim
    freq = (ROPE_THETA ** (-2.0 * np.arange(dim // 2, dtype=np.float64) / dim)).astype(np.float32)
    ck = cache_k.reshape(rows, local_slots, dim)
    cv = cache_v.reshape(rows, local_slots, dim)
    any_spec = pl.BlockSpec(memory_space=pltpu.HBM)
    vmem_spec = pl.BlockSpec(memory_space=pltpu.VMEM)
    chunks = rows // CHUNK
    nk, nv, part = pl.pallas_call(
        functools.partial(attn_kernel, sp_size),
        name="attend",
        out_shape=(
            jax.ShapeDtypeStruct((rows, local_slots, dim), BF16),
            jax.ShapeDtypeStruct((rows, local_slots, dim), BF16),
            pltpu.VMEM((sp_size, heads * rows // sp_size, dim + 128), F32),
        ),
        in_specs=[any_spec] * 9,
        out_specs=[any_spec, any_spec, vmem_spec],
        scratch_shapes=[
            pltpu.SMEM((rows,), jnp.int32),
            pltpu.VMEM((1, dim // 2), F32),
            pltpu.VMEM((rows, local_slots, dim), BF16),
            pltpu.VMEM((rows, local_slots, dim), BF16),
            pltpu.VMEM((rows, width), BF16),
            pltpu.VMEM((width,), BF16),
            pltpu.VMEM(w_q.shape, BF16),
            pltpu.VMEM(w_k.shape, BF16),
            pltpu.VMEM(w_v.shape, BF16),
            pltpu.VMEM((rows // 8, 8 * heads, dim), BF16),
            pltpu.VMEM((rows, dim), F32),
            pltpu.VMEM((rows, dim), F32),
            pltpu.VMEM((rows, 128), jnp.int32),
            pltpu.SemaphoreType.DMA((7,)),
            pltpu.SemaphoreType.DMA((chunks,)),
            pltpu.SemaphoreType.DMA((chunks,)),
            pltpu.SemaphoreType.DMA((chunks,)),
            pltpu.SemaphoreType.DMA((chunks,)),
        ],
        compiler_params=pltpu.CompilerParams(vmem_limit_bytes=VMEM_A),
        cost_estimate=pl.CostEstimate(flops=2 * rows * width * 1024, bytes_accessed=22 << 20, transcendentals=0),
    )(*in_hbm(positions, jnp.asarray(freq).reshape(1, -1), tokens, gain, w_q, w_k, w_v, ck, cv))
    return nk.reshape(cache_k.shape), nv.reshape(cache_v.shape), part


VMEM_A = 48 << 20


def partner(index, k):
    if k == 0:
        return index
    if k == 1:
        return index + 1 - 2 * lax.rem(index, 2)
    if k == 2:
        return lax.rem(index + 2, 4)
    return 3 - index


def finish_kernel(part_ref, tok_hbm, gain_hbm, wo_hbm, wg_hbm, wu_hbm, wd_hbm, out_ref,
                  wo, wg, wu, wd, tokv, gain, r1, y2, r2, r3, y4, r4, fin,
                  sem_w, s1, g1, s2, g2, s3, g3, s4, g4, s5z, g5z, s5y, g5y, s5c, g5c):
    s = lax.axis_index("sp")
    z = lax.axis_index("tp")
    width = wo.shape[1]
    wide = width // 2
    dim = part_ref.shape[2] - 128
    own_rows = part_ref.shape[1] // 2

    loads = [pltpu.make_async_copy(src, dst, sem_w.at[i]) for i, (src, dst) in enumerate((
        (tok_hbm.at[pl.ds(pl.multiple_of(s * own_rows, own_rows), own_rows)], tokv), (gain_hbm, gain),
        (wo_hbm, wo), (wg_hbm, wg), (wu_hbm, wu), (wd_hbm, wd)))]
    for copy in loads:
        copy.start()

    barrier = pltpu.get_barrier_semaphore()
    for k in (1, 2, 3):
        pl.semaphore_signal(barrier, inc=1, device_id={"tp": partner(z, k)}, device_id_type=MESH)
        pl.semaphore_signal(barrier, inc=1, device_id={"sp": partner(s, k)}, device_id_type=MESH)
    pl.semaphore_wait(barrier, 6)

    def send(src, dst, send_sem, recv_sem, **target):
        copy = pltpu.make_async_remote_copy(src_ref=src, dst_ref=dst, send_sem=send_sem, recv_sem=recv_sem,
                                            device_id=target, device_id_type=MESH)
        copy.start()
        return copy

    first = [send(part_ref.at[partner(s, k)], r1.at[k - 1], s1.at[k - 1], g1.at[k - 1], sp=partner(s, k)) for k in (3, 2, 1)]

    sub = lax.broadcasted_iota(jnp.int32, (8, wide), 0)
    low = sub < 4

    def piece(left, right, d):
        t = d // 2
        a, b = left[8 * t:8 * t + 8], right[8 * t:8 * t + 8]
        mask = low[:, :a.shape[1]]
        return jnp.where(mask, a, b) if d % 2 == 0 else jnp.where(mask, b, a)

    def swap(x):
        return jnp.concatenate([pltpu.roll(x[8 * t:8 * t + 8], 4, 0) for t in range(x.shape[0] // 8)], axis=0)

    def rows_of(four):
        lefts, rights = [], []
        for t in range(2):
            a, b = four[2 * t], four[2 * t + 1]
            mask = low[:, :a.shape[1]]
            lefts.append(jnp.where(mask, a, b))
            rights.append(pltpu.roll(jnp.where(mask, b, a), 4, 0))
        return jnp.concatenate(lefts, axis=0), jnp.concatenate(rights, axis=0)

    loads[0].wait()
    loads[1].wait()
    tok = tokv[...].astype(F32)
    tok_l, tok_r = tok[:, :wide], swap(tok[:, wide:])
    tok_piece = piece(tok_l, tok_r, 0)
    for d in (1, 2, 3):
        tok_piece = jnp.where(z == d, piece(tok_l, tok_r, d), tok_piece)
    gain_row = gain[...].astype(F32).reshape(1, -1)
    even = lax.rem(z, 2) == 0
    gain_piece = jnp.where(jnp.where(even, sub, 7 - sub) < 4, gain_row[:, :wide], gain_row[:, wide:])

    for copy in first:
        copy.wait_recv()
    parts = [part_ref[s], r1[0], r1[1], r1[2]]
    tops = [p[:, dim:dim + 1] for p in parts]
    sums = [p[:, dim + 64:dim + 65] for p in parts]
    top = jnp.maximum(jnp.maximum(tops[0], tops[1]), jnp.maximum(tops[2], tops[3]))
    scales = [jnp.exp(t - top) for t in tops]
    total = sum(f * l for f, l in zip(scales, sums))
    mixed = sum(f * p[:, :dim] for f, p in zip(scales, parts)) / total
    att = jnp.concatenate([mixed[:own_rows], mixed[own_rows:]], axis=1)
    att_swapped = swap(att).astype(BF16)
    att = att.astype(BF16)

    loads[2].wait()
    second = []
    for c, (at, size) in enumerate(CUT_O):
        left = jnp.dot(att, wo[:, at:at + size], preferred_element_type=F32)
        right = jnp.dot(att_swapped, wo[:, wide + at:wide + at + size], preferred_element_type=F32)
        for d in range(4):
            y2[d, :, at:at + size] = piece(left, right, d)
        for k in (3, 2, 1):
            second.append(send(y2.at[partner(z, k), :, pl.ds(at, size)], r2.at[k - 1, :, pl.ds(at, size)],
                               s2.at[k - 1, c], g2.at[k - 1, c], tp=partner(z, k)))
    for copy in second:
        copy.wait_recv()
    hidden = (tok_piece + (y2[z] + r2[0] + r2[1] + r2[2])).astype(BF16).astype(F32)
    squares = jnp.sum(hidden * hidden, axis=-1, keepdims=True)
    squares = jnp.broadcast_to(squares, (8, 128))
    squares = squares + pltpu.roll(squares, 4, 0)
    inv_rms = lax.rsqrt(squares[:, :1] / width + NORM_EPS)
    r3[z] = (hidden * inv_rms * gain_piece).astype(BF16).astype(F32)

    third = []
    for c, (at, size) in enumerate(CUT_M):
        for k in (3, 2, 1):
            third.append(send(r3.at[z, :, pl.ds(at, size)], r3.at[z, :, pl.ds(at, size)], s3.at[k - 1, c], g3.at[k - 1, c],
                              tp=partner(z, k)))
    loads[3].wait()
    loads[4].wait()
    gate = up = None
    for c, (at, size) in enumerate(CUT_M):
        for copy in third[3 * c:3 * c + 3]:
            copy.wait_recv()
        left, right = rows_of([r3[d, :, at:at + size] for d in range(4)])
        left, right = left.astype(BF16), right.astype(BF16)
        pair = []
        for w in (wg, wu):
            pair.append(jnp.dot(left, w[at:at + size, :], preferred_element_type=F32)
                        + jnp.dot(right, w[wide + at:wide + at + size, :], preferred_element_type=F32))
        gate = pair[0] if gate is None else gate + pair[0]
        up = pair[1] if up is None else up + pair[1]
    act = gate * (1.0 / (1.0 + jnp.exp(-gate))) * up
    act = act.astype(BF16)
    act_swapped = swap(act.astype(F32)).astype(BF16)

    loads[5].wait()
    fourth = []
    for c, (at, size) in enumerate(CUT_D):
        left = jnp.dot(act, wd[:, at:at + size], preferred_element_type=F32)
        right = jnp.dot(act_swapped, wd[:, wide + at:wide + at + size], preferred_element_type=F32)
        for d in range(4):
            y4[d, :, at:at + size] = piece(left, right, d)
        for k in (3, 2, 1):
            fourth.append(send(y4.at[partner(z, k), :, pl.ds(at, size)], r4.at[k - 1, :, pl.ds(at, size)],
                               s4.at[k - 1, c], g4.at[k - 1, c], tp=partner(z, k)))

    along, across, beside = {}, {}, {}
    for c, (at, size) in enumerate(CUT_D):
        for copy in fourth[3 * c:3 * c + 3]:
            copy.wait_recv()
        span = pl.ds(at, size)
        total = y4[z, :, at:at + size] + r4[0, :, at:at + size] + r4[1, :, at:at + size] + r4[2, :, at:at + size]
        fin[s, z, :, at:at + size] = (hidden[:, at:at + size] + total).astype(BF16).astype(F32)
        mine = fin.at[s, z, :, span]
        for k in (3, 2, 1):
            along[c, k] = send(mine, mine, s5z.at[k - 1, c], g5z.at[k - 1, c], tp=partner(z, k))
        across[c, 0] = send(mine, mine, s5y.at[0, c], g5y.at[0, c], sp=partner(s, 2))
        beside[c, 0] = send(mine, mine, s5c.at[0, c], g5c.at[0, c], sp=partner(s, 1))
    for c, (at, size) in enumerate(CUT_D):
        span = pl.ds(at, size)
        for k in (1, 2, 3):
            along[c, k].wait_recv()
            came = fin.at[s, partner(z, k), :, span]
            across[c, k] = send(came, came, s5y.at[k, c], g5y.at[k, c], sp=partner(s, 2))
            beside[c, k] = send(came, came, s5c.at[k, c], g5c.at[k, c], sp=partner(s, 1))
    for c, (at, size) in enumerate(CUT_D):
        span = pl.ds(at, size)
        for k in range(4):
            across[c, k].wait_recv()
            came = fin.at[partner(s, 2), partner(z, k), :, span]
            beside[c, 4 + k] = send(came, came, s5c.at[4 + k, c], g5c.at[4 + k, c], sp=partner(s, 1))
    for copy in beside.values():
        copy.wait_recv()
    for r in range(4):
        left, right = rows_of([fin[r, d] for d in range(4)])
        out_ref[pl.ds(own_rows * r, own_rows), 0:wide] = left.astype(BF16)
        out_ref[pl.ds(own_rows * r, own_rows), wide:width] = right.astype(BF16)
    for copy in first + second + third + fourth + list(along.values()) + list(across.values()) + list(beside.values()):
        copy.wait_send()


MESH = pl.DeviceIdType.MESH
CUT_O = ((0, 256), (256, 1024))
CUT_M = ((0, 256), (256, 512), (768, 512))
CUT_D = ((0, 256), (256, 512), (768, 512))


def finish(part, tokens, gain, w_o, w_gate, w_up, w_down):
    rows, width = tokens.shape
    hbm = pl.BlockSpec(memory_space=pltpu.HBM)
    vmem = pl.BlockSpec(memory_space=pltpu.VMEM)
    own = part.shape[1] // 2
    half = width // 2
    dma = pltpu.SemaphoreType.DMA
    return pl.pallas_call(
        finish_kernel,
        name="finish",
        out_shape=pltpu.VMEM((rows, width), BF16),
        in_specs=[vmem] + [hbm] * 6,
        out_specs=vmem,
        scratch_shapes=[
            pltpu.VMEM(w_o.shape, BF16),
            pltpu.VMEM(w_gate.shape, BF16),
            pltpu.VMEM(w_up.shape, BF16),
            pltpu.VMEM(w_down.shape, BF16),
            pltpu.VMEM((own, width), BF16),
            pltpu.VMEM((width,), BF16),
            pltpu.VMEM((3,) + part.shape[1:], F32),
            pltpu.VMEM((4, 8, half), F32),
            pltpu.VMEM((3, 8, half), F32),
            pltpu.VMEM((4, 8, half), F32),
            pltpu.VMEM((4, 8, half), F32),
            pltpu.VMEM((3, 8, half), F32),
            pltpu.VMEM((4, 4, 8, half), F32),
            dma((6,)),
            dma((3,)), dma((3,)),
            dma((3, len(CUT_O))), dma((3, len(CUT_O))),
            dma((3, len(CUT_M))), dma((3, len(CUT_M))),
            dma((3, len(CUT_D))), dma((3, len(CUT_D))),
            dma((3, len(CUT_D))), dma((3, len(CUT_D))),
            dma((4, len(CUT_D))), dma((4, len(CUT_D))),
            dma((8, len(CUT_D))), dma((8, len(CUT_D))),
        ],
        compiler_params=pltpu.CompilerParams(collective_id=0, has_side_effects=True, vmem_limit_bytes=VMEM_B),
        cost_estimate=pl.CostEstimate(flops=2 * 16 * width * 2560 * 3, bytes_accessed=42 << 20, transcendentals=0),
    )(part, *in_hbm(tokens, gain, w_o, w_gate, w_up, w_down))


VMEM_B = 48 << 20


def solution(mesh):
    sp_size = mesh.shape["sp"]
    cache_spec = P("dp", "sp", "tp", None)
    row_spec = P("dp", None)
    col_spec = P(None, "tp")
    in_specs = (row_spec, P("dp"), cache_spec, cache_spec, P(None), col_spec, col_spec, col_spec, P("tp", None), P(None), col_spec, col_spec, P("tp", None))
    out_specs = (row_spec, cache_spec, cache_spec)

    def local_step(tokens, positions, cache_k, cache_v, attn_gain, w_q, w_k, w_v, w_o, mlp_gain, w_gate, w_up, w_down):
        new_k, new_v, part = attend(tokens, positions, cache_k, cache_v, attn_gain, w_q, w_k, w_v, sp_size)
        layer_out = finish(part, tokens, mlp_gain, w_o, w_gate, w_up, w_down)
        return layer_out, new_k, new_v

    return jax.shard_map(local_step, mesh=mesh, in_specs=in_specs, out_specs=out_specs, check_vma=False)
```

```python
import functools
import math

import jax
import jax.numpy as jnp
import numpy as np
from jax import lax
from jax.experimental import pallas as pl
from jax.experimental.pallas import tpu as pltpu
from jax.sharding import PartitionSpec as P

NORM_EPS = 1e-5
ROPE_THETA = 10000.0
F32 = jnp.float32
BF16 = jnp.bfloat16
CHUNK = 16


def attn_kernel(sp_size, pos_hbm, freq_hbm, tok_hbm, gain_hbm, wq_hbm, wk_hbm, wv_hbm, ck_hbm, cv_hbm,
                nk_hbm, nv_hbm, part_ref, pos_ref, freq_ref, nk_ref, nv_ref, tok, gain, wq, wk, wv, qs, knew, vnew, posm,
                sem_w, sem_k, sem_v, sem_ko, sem_vo):
    rows = tok.shape[0]
    local_slots = nk_ref.shape[1]
    dim = nk_ref.shape[2]
    half = dim // 2
    slots = local_slots * sp_size
    chunks = rows // CHUNK
    base = lax.axis_index("sp") * local_slots

    loads = [pltpu.make_async_copy(src, dst, sem_w.at[i]) for i, (src, dst) in enumerate(
        ((tok_hbm, tok), (gain_hbm, gain), (wk_hbm, wk), (wv_hbm, wv), (wq_hbm, wq), (pos_hbm, pos_ref), (freq_hbm, freq_ref)))]
    for i in (5, 6, 0, 1, 2, 3, 4):
        loads[i].start()
    k_loads, v_loads, k_stores, v_stores = [], [], [], []
    for c in range(chunks):
        span = pl.ds(c * CHUNK, CHUNK)
        k_loads.append(pltpu.make_async_copy(ck_hbm.at[span], nk_ref.at[span], sem_k.at[c]))
        v_loads.append(pltpu.make_async_copy(cv_hbm.at[span], nv_ref.at[span], sem_v.at[c]))
        k_stores.append(pltpu.make_async_copy(nk_ref.at[span], nk_hbm.at[span], sem_ko.at[c]))
        v_stores.append(pltpu.make_async_copy(nv_ref.at[span], nv_hbm.at[span], sem_vo.at[c]))

    loads[5].wait()
    loads[6].wait()
    sub = lax.broadcasted_iota(jnp.int32, (8, 128), 0)
    for g in range(rows // 8):
        acc = jnp.zeros((8, 128), jnp.int32)
        for r in range(8):
            acc = jnp.where(sub == r, pos_ref[8 * g + r], acc)
        posm[pl.ds(8 * g, 8), :] = acc
    angles = posm[...].astype(F32) * freq_ref[...]
    cos = jnp.cos(angles)
    sin = jnp.sin(angles)

    loads[0].wait()
    loads[1].wait()
    wide = tok[...].astype(F32)
    inv_rms = lax.rsqrt(jnp.mean(wide * wide, axis=-1, keepdims=True) + NORM_EPS)
    normed = (wide * inv_rms * gain[...].astype(F32).reshape(1, -1)).astype(BF16)

    def fetch(c):
        if c < chunks:
            k_loads[c].start()
            v_loads[c].start()

    def rope(lin):
        a, b = lin[:, :half], lin[:, half:]
        return jnp.concatenate([a * cos - b * sin, b * cos + a * sin], axis=-1)

    loads[2].wait()
    fetch(0)
    knew[...] = rope(jnp.dot(normed, wk[...], preferred_element_type=F32)).astype(BF16).astype(F32)
    loads[3].wait()
    vnew[...] = jnp.dot(normed, wv[...], preferred_element_type=F32).astype(BF16).astype(F32)
    loads[4].wait()
    fetch(1)
    heads = wq.shape[1] // dim
    q_lin = jnp.dot(normed, wq[...], preferred_element_type=F32)
    q_rot = [rope(q_lin[:, h * dim:(h + 1) * dim]) for h in range(heads)]
    for g in range(rows // 8):
        qs[g] = jnp.concatenate([q_rot[h][8 * g:8 * g + 8] for h in range(heads)], axis=0).astype(BF16)

    sub16 = lax.broadcasted_iota(jnp.int32, (16, dim), 0)
    lane = lax.broadcasted_iota(jnp.int32, (16, local_slots), 1) + base
    lane128 = lax.broadcasted_iota(jnp.int32, (16, 128), 1)

    def patch(ref, new_ref, b, offset):
        inside = jnp.clip(offset, 0, local_slots - 1)
        start = pl.multiple_of((inside // 16) * 16, 16)
        old = ref[b, pl.ds(start, 16), :].astype(F32)
        ref[b, pl.ds(start, 16), :] = jnp.where(sub16 == offset - start, new_ref[pl.ds(b, 1), :], old).astype(BF16)

    for c in range(chunks):
        offsets = [jnp.bitwise_and(pos_ref[c * CHUNK + j], slots - 1) - base for j in range(CHUNK)]
        k_loads[c].wait()
        fetch(c + 2)
        for j in range(CHUNK):
            patch(nk_ref, knew, c * CHUNK + j, offsets[j])
        k_stores[c].start()
        probs = []
        for g in range(c * CHUNK // 8, (c + 1) * CHUNK // 8):
            query = qs[g]
            scores = jnp.zeros((16, local_slots), F32)
            for j in range(8):
                one = lax.dot_general(query, nk_ref[8 * g + j], (((1,), (1,)), ((), ())), preferred_element_type=F32)
                scores = jnp.where(jnp.bitwise_and(sub16, 7) == j, one, scores)
            scores = scores * (1.0 / math.sqrt(dim))
            pos8 = posm[pl.ds(8 * g, 8), :]
            pos16 = jnp.concatenate([pos8, pos8], axis=0)
            limit = jnp.where(pos16 >= slots - 1, slots, pos16)
            valid = lane <= jnp.concatenate([limit] * (local_slots // 128), axis=1)
            top = jnp.max(jnp.where(valid, scores, -jnp.inf), axis=-1, keepdims=True)
            safe = jnp.where(top == -jnp.inf, 0.0, top)
            weights = jnp.exp(jnp.where(valid, scores - safe, -jnp.inf))
            total = jnp.sum(weights, axis=-1, keepdims=True)
            probs.append((g, weights.astype(BF16), top, total))
        v_loads[c].wait()
        for j in range(CHUNK):
            patch(nv_ref, vnew, c * CHUNK + j, offsets[j])
        v_stores[c].start()
        for g, weights, top, total in probs:
            out = jnp.zeros((16, dim), F32)
            for j in range(8):
                one = jnp.dot(weights, nv_ref[8 * g + j], preferred_element_type=F32)
                out = jnp.where(jnp.bitwise_and(sub16, 7) == j, one, out)
            stats = jnp.where(lane128 < 64, top, total)
            dest, upper = g // 2, g % 2
            for h in range(heads):
                span = pl.ds(16 * h + 8 * upper, 8)
                part_ref[dest, span, 0:dim] = out[8 * h:8 * h + 8]
                part_ref[dest, span, dim:dim + 128] = stats[8 * h:8 * h + 8]
    for copy in k_stores + v_stores:
        copy.wait()


def in_hbm(*arrays):
    return [pltpu.with_memory_space_constraint(x, pltpu.HBM) for x in arrays]


def attend(tokens, positions, cache_k, cache_v, gain, w_q, w_k, w_v, sp_size):
    rows, width = tokens.shape
    _, local_slots, _, dim = cache_k.shape
    heads = w_q.shape[1] // dim
    freq = (ROPE_THETA ** (-2.0 * np.arange(dim // 2, dtype=np.float64) / dim)).astype(np.float32)
    ck = cache_k.reshape(rows, local_slots, dim)
    cv = cache_v.reshape(rows, local_slots, dim)
    any_spec = pl.BlockSpec(memory_space=pltpu.HBM)
    vmem_spec = pl.BlockSpec(memory_space=pltpu.VMEM)
    chunks = rows // CHUNK
    nk, nv, part = pl.pallas_call(
        functools.partial(attn_kernel, sp_size),
        name="attend",
        out_shape=(
            jax.ShapeDtypeStruct((rows, local_slots, dim), BF16),
            jax.ShapeDtypeStruct((rows, local_slots, dim), BF16),
            pltpu.VMEM((sp_size, heads * rows // sp_size, dim + 128), F32),
        ),
        in_specs=[any_spec] * 9,
        out_specs=[any_spec, any_spec, vmem_spec],
        scratch_shapes=[
            pltpu.SMEM((rows,), jnp.int32),
            pltpu.VMEM((1, dim // 2), F32),
            pltpu.VMEM((rows, local_slots, dim), BF16),
            pltpu.VMEM((rows, local_slots, dim), BF16),
            pltpu.VMEM((rows, width), BF16),
            pltpu.VMEM((width,), BF16),
            pltpu.VMEM(w_q.shape, BF16),
            pltpu.VMEM(w_k.shape, BF16),
            pltpu.VMEM(w_v.shape, BF16),
            pltpu.VMEM((rows // 8, 8 * heads, dim), BF16),
            pltpu.VMEM((rows, dim), F32),
            pltpu.VMEM((rows, dim), F32),
            pltpu.VMEM((rows, 128), jnp.int32),
            pltpu.SemaphoreType.DMA((7,)),
            pltpu.SemaphoreType.DMA((chunks,)),
            pltpu.SemaphoreType.DMA((chunks,)),
            pltpu.SemaphoreType.DMA((chunks,)),
            pltpu.SemaphoreType.DMA((chunks,)),
        ],
        compiler_params=pltpu.CompilerParams(vmem_limit_bytes=VMEM_A),
        cost_estimate=pl.CostEstimate(flops=2 * rows * width * 1024, bytes_accessed=22 << 20, transcendentals=0),
    )(*in_hbm(positions, jnp.asarray(freq).reshape(1, -1), tokens, gain, w_q, w_k, w_v, ck, cv))
    return nk.reshape(cache_k.shape), nv.reshape(cache_v.shape), part


VMEM_A = 48 << 20


def partner(index, k):
    if k == 0:
        return index
    if k == 1:
        return index + 1 - 2 * lax.rem(index, 2)
    if k == 2:
        return lax.rem(index + 2, 4)
    return 3 - index


def finish_kernel(part_ref, tok_hbm, gain_hbm, wo_hbm, wg_hbm, wu_hbm, wd_hbm, out_ref,
                  wo, wg, wu, wd, tokv, gain, r1, y2, r2, hid, norm, ms, y4, r4, fin,
                  sem_w, s1, g1, s2, g2, s3, g3, s4, g4, s5z, g5z, s5y, g5y, s5c, g5c):
    s = lax.axis_index("sp")
    z = lax.axis_index("tp")
    line, core = s // 2, lax.rem(s, 2)
    width = wo.shape[1]
    dim = part_ref.shape[2] - 128
    own_rows = part_ref.shape[1] // 2
    owner = (core == 1) & ((z == 1) | (z == 2))
    tile = jnp.clip(z - 1, 0, 1)

    loads = [pltpu.make_async_copy(src, dst, sem_w.at[i]) for i, (src, dst) in enumerate((
        (tok_hbm.at[pl.ds(pl.multiple_of(2 * line * own_rows, own_rows), 2 * own_rows)], tokv), (gain_hbm, gain),
        (wo_hbm, wo), (wg_hbm, wg), (wu_hbm, wu), (wd_hbm, wd)))]
    for copy in loads:
        copy.start()

    def is_owner(t):
        return (core == 1) & (z == t + 1)

    barrier = pltpu.get_barrier_semaphore()
    for k in (1, 2, 3):
        pl.semaphore_signal(barrier, inc=1, device_id={"sp": partner(s, k), "tp": z}, device_id_type=MESH)
    for t in range(2):
        @pl.when(z != t + 1)
        def _():
            pl.semaphore_signal(barrier, inc=1, device_id={"sp": 2 * line + 1, "tp": t + 1}, device_id_type=MESH)

    @pl.when(owner)
    def _():
        for k in (1, 2, 3):
            pl.semaphore_signal(barrier, inc=1, device_id={"sp": 2 * line, "tp": partner(z, k)}, device_id_type=MESH)
        for k in (1, 2):
            pl.semaphore_signal(barrier, inc=1, device_id={"sp": 2 * line + 1, "tp": partner(z, k)}, device_id_type=MESH)

    middle = (z == 1) | (z == 2)
    pl.semaphore_wait(barrier, jnp.where(middle, jnp.where(core == 1, 9, 4), 5))

    def remote(src, dst, send_sem, recv_sem, sp, tp):
        return pltpu.make_async_remote_copy(src_ref=src, dst_ref=dst, send_sem=send_sem, recv_sem=recv_sem,
                                            device_id={"sp": sp, "tp": tp}, device_id_type=MESH)

    first = [remote(part_ref.at[partner(s, k)], r1.at[k - 1], s1.at[k - 1], g1.at[k - 1], partner(s, k), z) for k in (3, 2, 1)]
    for copy in first:
        copy.start()

    def to_owner(t, c, cut, rows, sums, send_sem, recv_sem):
        span = pl.ds(*cut[c])
        return remote(rows.at[t, :, span], sums.at[core, z, :, span], send_sem.at[t, c], recv_sem.at[core, z, c], 2 * line + 1, t + 1)

    def send_sums(value, c, cut, rows, sums, send_sem, recv_sem):
        at, size = cut[c]
        for t in range(2):
            rows[t, :, at:at + size] = value[8 * t:8 * t + 8]
        for t in range(2):
            @pl.when(jnp.logical_not(is_owner(t)))
            def _():
                to_owner(t, c, cut, rows, sums, send_sem, recv_sem).start()

    def wait_sums(c, cut, rows, sums, send_sem, recv_sem):
        at, size = cut[c]
        span = pl.ds(at, size)
        sums[1, z, :, at:at + size] = rows[tile, :, at:at + size]
        for b in range(2):
            for k in (1, 3, 2, 0):
                if b == 0 or k:
                    far = partner(z, k)
                    remote(rows.at[0, :, span], sums.at[b, far, :, span], send_sem.at[0, c], recv_sem.at[b, far, c], 2 * line + b, far).wait_recv()
        return [sums[b, 0, :, at:at + size] + sums[b, 1, :, at:at + size] + sums[b, 2, :, at:at + size] + sums[b, 3, :, at:at + size]
                for b in range(2)]

    def sent_sums(cut, rows, sums, send_sem, recv_sem):
        for t in range(2):
            @pl.when(jnp.logical_not(is_owner(t)))
            def _():
                for c in range(len(cut)):
                    to_owner(t, c, cut, rows, sums, send_sem, recv_sem).wait_send()

    for copy in first:
        copy.wait_recv()
    parts = [part_ref[s], r1[0], r1[1], r1[2]]
    tops = [p[:, dim:dim + 1] for p in parts]
    sums = [p[:, dim + 64:dim + 65] for p in parts]
    top = jnp.maximum(jnp.maximum(tops[0], tops[1]), jnp.maximum(tops[2], tops[3]))
    scales = [jnp.exp(t - top) for t in tops]
    total = sum(f * l for f, l in zip(scales, sums))
    mixed = sum(f * p[:, :dim] for f, p in zip(scales, parts)) / total
    att = jnp.concatenate([mixed[:own_rows], mixed[own_rows:]], axis=1).astype(BF16)

    loads[2].wait()
    for c, (at, size) in enumerate(CUT_O):
        send_sums(jnp.dot(att, wo[:, at:at + size], preferred_element_type=F32), c, CUT_O, y2, r2, s2, g2)

    def spread(b, k, c):
        span = pl.ds(*CUT_M[c])
        return remote(norm.at[b, :, span], ms.at[tile, :, span], s3.at[b, k, c], g3.at[tile, c], 2 * line + b, partner(z, k))

    loads[0].wait()
    loads[1].wait()

    @pl.when(owner)
    def _():
        halves = [wait_sums(c, CUT_O, y2, r2, s2, g2) for c in range(len(CUT_O))]
        for b in range(2):
            tok = tokv[pl.ds(own_rows * b, own_rows), :].astype(F32)
            tok = jnp.where(tile == 0, tok[0:8], tok[8:16])
            hidden = (tok + jnp.concatenate([h[b] for h in halves], axis=1)).astype(BF16).astype(F32)
            inv_rms = lax.rsqrt(jnp.mean(hidden * hidden, axis=-1, keepdims=True) + NORM_EPS)
            normed = (hidden * inv_rms * gain[...].astype(F32).reshape(1, -1)).astype(BF16).astype(F32)
            hid[b] = hidden
            norm[b] = normed
            if b == 1:
                ms[tile] = normed
        for c in range(len(CUT_M)):
            for k in (2, 3, 1, 0):
                for b in (0, 1):
                    if b == 0 or k:
                        spread(b, k, c).start()

    loads[3].wait()
    loads[4].wait()
    gate = up = None
    for c, (at, size) in enumerate(CUT_M):
        span = pl.ds(at, size)
        for t in range(2):
            @pl.when(jnp.logical_not(is_owner(t)))
            def _():
                remote(norm.at[0, :, span], ms.at[t, :, span], s3.at[0, 0, c], g3.at[t, c], 2 * line + 1, t + 1).wait_recv()
        rows = jnp.concatenate([ms[0, :, at:at + size], ms[1, :, at:at + size]], axis=0).astype(BF16)
        pair = [jnp.dot(rows, w[at:at + size, :], preferred_element_type=F32) for w in (wg, wu)]
        gate = pair[0] if gate is None else gate + pair[0]
        up = pair[1] if up is None else up + pair[1]
    act = gate * (1.0 / (1.0 + jnp.exp(-gate))) * up
    act = act.astype(BF16)

    loads[5].wait()
    for c, (at, size) in enumerate(CUT_D):
        send_sums(jnp.dot(act, wd[:, at:at + size], preferred_element_type=F32), c, CUT_D, y4, r4, s4, g4)

    def along(t, k, c):
        span = pl.ds(*CUT_D[c])
        rows = fin.at[line, t, :, :, span]
        return remote(rows, rows, s5z.at[k, c], g5z.at[t, c], s, partner(z, k))

    def across(t, c):
        span = pl.ds(*CUT_D[c])
        rows = fin.at[line, t, :, :, span]
        return remote(rows, rows, s5y.at[t, c], g5y.at[t, c], partner(s, 2), z)

    def beside(far, t, c):
        span = pl.ds(*CUT_D[c])
        rows = fin.at[line if far == 0 else 1 - line, t, :, :, span]
        return remote(rows, rows, s5c.at[far, t, c], g5c.at[far, t, c], partner(s, 1), z)

    @pl.when(owner)
    def _():
        for c, (at, size) in enumerate(CUT_D):
            totals = wait_sums(c, CUT_D, y4, r4, s4, g4)
            for b in range(2):
                fin[line, tile, b, :, at:at + size] = (hid[b, :, at:at + size] + totals[b]).astype(BF16).astype(F32)
            for k in (2, 3, 1):
                along(tile, k, c).start()
            across(tile, c).start()
            beside(0, tile, c).start()

    @pl.when(core == 1)
    def _():
        for c in range(len(CUT_D)):
            for t in range(2):
                @pl.when(z != t + 1)
                def _():
                    along(t, 1, c).wait_recv()
                    across(t, c).start()
                    beside(0, t, c).start()
        for c in range(len(CUT_D)):
            for t in range(2):
                span = pl.ds(*CUT_D[c])
                rows = fin.at[1 - line, t, :, :, span]
                remote(rows, rows, s5y.at[t, c], g5y.at[t, c], partner(s, 2), z).wait_recv()
                beside(1, t, c).start()

    @pl.when(core == 0)
    def _():
        for far in range(2):
            for c in range(len(CUT_D)):
                for t in range(2):
                    beside(far, t, c).wait_recv()

    for y in range(2):
        for b in range(2):
            out_ref[pl.ds(own_rows * (2 * y + b), own_rows), :] = jnp.concatenate([fin[y, 0, b], fin[y, 1, b]], axis=0).astype(BF16)

    for copy in first:
        copy.wait_send()
    sent_sums(CUT_O, y2, r2, s2, g2)
    sent_sums(CUT_D, y4, r4, s4, g4)

    @pl.when(owner)
    def _():
        for c in range(len(CUT_M)):
            for k in range(4):
                for b in range(2):
                    if b == 0 or k:
                        spread(b, k, c).wait_send()
        for c in range(len(CUT_D)):
            for k in (1, 2, 3):
                along(tile, k, c).wait_send()

    @pl.when(core == 1)
    def _():
        for c in range(len(CUT_D)):
            for t in range(2):
                across(t, c).wait_send()
                beside(0, t, c).wait_send()
                beside(1, t, c).wait_send()


MESH = pl.DeviceIdType.MESH
CUT_O = ((0, 512), (512, 2048))
CUT_M = ((0, 512), (512, 512), (1024, 512), (1536, 512), (2048, 512))
CUT_D = ((0, 512), (512, 512), (1024, 512), (1536, 512), (2048, 512))


def finish(part, tokens, gain, w_o, w_gate, w_up, w_down):
    rows, width = tokens.shape
    hbm = pl.BlockSpec(memory_space=pltpu.HBM)
    vmem = pl.BlockSpec(memory_space=pltpu.VMEM)
    own = part.shape[1] // 2
    dma = pltpu.SemaphoreType.DMA
    cut_o, cut_m, cut_d = len(CUT_O), len(CUT_M), len(CUT_D)
    return pl.pallas_call(
        finish_kernel,
        name="finish",
        out_shape=pltpu.VMEM((rows, width), BF16),
        in_specs=[vmem] + [hbm] * 6,
        out_specs=vmem,
        scratch_shapes=[
            pltpu.VMEM(w_o.shape, BF16),
            pltpu.VMEM(w_gate.shape, BF16),
            pltpu.VMEM(w_up.shape, BF16),
            pltpu.VMEM(w_down.shape, BF16),
            pltpu.VMEM((2 * own, width), BF16),
            pltpu.VMEM((width,), BF16),
            pltpu.VMEM((3,) + part.shape[1:], F32),
            pltpu.VMEM((2, 8, width), F32),
            pltpu.VMEM((2, 4, 8, width), F32),
            pltpu.VMEM((2, 8, width), F32),
            pltpu.VMEM((2, 8, width), F32),
            pltpu.VMEM((2, 8, width), F32),
            pltpu.VMEM((2, 8, width), F32),
            pltpu.VMEM((2, 4, 8, width), F32),
            pltpu.VMEM((2, 2, 2, 8, width), F32),
            dma((6,)),
            dma((3,)), dma((3,)),
            dma((2, cut_o)), dma((2, 4, cut_o)),
            dma((2, 4, cut_m)), dma((2, cut_m)),
            dma((2, cut_d)), dma((2, 4, cut_d)),
            dma((4, cut_d)), dma((2, cut_d)),
            dma((2, cut_d)), dma((2, cut_d)),
            dma((2, 2, cut_d)), dma((2, 2, cut_d)),
        ],
        compiler_params=pltpu.CompilerParams(collective_id=0, has_side_effects=True, vmem_limit_bytes=VMEM_B),
        cost_estimate=pl.CostEstimate(flops=2 * 16 * width * 2560 * 3, bytes_accessed=42 << 20, transcendentals=0),
    )(part, *in_hbm(tokens, gain, w_o, w_gate, w_up, w_down))


VMEM_B = 50 << 20


def solution(mesh):
    sp_size = mesh.shape["sp"]
    cache_spec = P("dp", "sp", "tp", None)
    row_spec = P("dp", None)
    col_spec = P(None, "tp")
    in_specs = (row_spec, P("dp"), cache_spec, cache_spec, P(None), col_spec, col_spec, col_spec, P("tp", None), P(None), col_spec, col_spec, P("tp", None))
    out_specs = (row_spec, cache_spec, cache_spec)

    def local_step(tokens, positions, cache_k, cache_v, attn_gain, w_q, w_k, w_v, w_o, mlp_gain, w_gate, w_up, w_down):
        new_k, new_v, part = attend(tokens, positions, cache_k, cache_v, attn_gain, w_q, w_k, w_v, sp_size)
        layer_out = finish(part, tokens, mlp_gain, w_o, w_gate, w_up, w_down)
        return layer_out, new_k, new_v

    return jax.shard_map(local_step, mesh=mesh, in_specs=in_specs, out_specs=out_specs, check_vma=False)
```

```python
import functools
import math

import jax
import jax.numpy as jnp
import numpy as np
from jax import lax
from jax.experimental import pallas as pl
from jax.experimental.pallas import tpu as pltpu
from jax.sharding import PartitionSpec as P

NORM_EPS = 1e-5
ROPE_THETA = 10000.0
F32 = jnp.float32
BF16 = jnp.bfloat16
CHUNK = 16


def in_hbm(*arrays):
    return [pltpu.with_memory_space_constraint(x, pltpu.HBM) for x in arrays]


def partner(index, k):
    if k == 0:
        return index
    if k == 1:
        return index + 1 - 2 * lax.rem(index, 2)
    if k == 2:
        return lax.rem(index + 2, 4)
    return 3 - index


def layer_kernel(pos_hbm, freq_hbm, tok_hbm, gain_hbm, wq_hbm, wk_hbm, wv_hbm, ck_hbm, cv_hbm,
                 gain2_hbm, wo_hbm, wg_hbm, wu_hbm, wd_hbm, nk_ref, nv_ref, knew, vnew, out_ref,
                 pos_ref, freq_ref, tok, gain, gain2, qs, posm, part, wo, wg, wu, wd, r1, y2, r2, norm, ms, fin, normed,
                 sem_w, sem_l, sem_k, sem_v, s1, g1, s2, g2, s3, g3, s4, g4, s5z, g5z, s5y, g5y, s5c, g5c):
    s = lax.axis_index("sp")
    z = lax.axis_index("tp")
    line, core = s // 2, lax.rem(s, 2)
    width = wo.shape[1]
    own_rows = CHUNK
    rows = tok.shape[0]
    local_slots, dim = nk_ref.shape[1:]
    half = dim // 2
    chunks = rows // CHUNK
    slots = local_slots * chunks
    base = s * local_slots
    kv_width, q_width = wk_hbm.shape[1], wq_hbm.shape[1]
    wk, wv, wq = wd.at[:, 0:kv_width], wd.at[:, kv_width:2 * kv_width], wd.at[:, 2 * kv_width:2 * kv_width + q_width]
    owner = (core == 1) & ((z == 1) | (z == 2))
    tile = jnp.clip(z - 1, 0, 1)

    loads = [pltpu.make_async_copy(src, dst, sem_w.at[i]) for i, (src, dst) in enumerate((
        (tok_hbm, tok), (gain_hbm, gain), (wk_hbm, wk), (wv_hbm, wv), (wq_hbm, wq), (pos_hbm, pos_ref), (freq_hbm, freq_ref),
        (gain2_hbm, gain2)))]
    for i in (5, 6, 0, 1, 2, 3, 4, 7):
        loads[i].start()
    late = [pltpu.make_async_copy(src, dst, sem_l.at[i]) for i, (src, dst) in enumerate((
        (wo_hbm, wo), (wg_hbm, wg), (wu_hbm, wu), (wd_hbm, wd)))]
    order = [partner(s, k) for k in (3, 2, 1, 0)]
    k_loads, v_loads = [], []
    for c, d in enumerate(order):
        span = pl.ds(pl.multiple_of(d * CHUNK, CHUNK), CHUNK)
        k_loads.append(pltpu.make_async_copy(ck_hbm.at[span], nk_ref.at[span], sem_k.at[c]))
        v_loads.append(pltpu.make_async_copy(cv_hbm.at[span], nv_ref.at[span], sem_v.at[c]))

    def is_owner(t):
        return (core == 1) & (z == t + 1)

    barrier = pltpu.get_barrier_semaphore()
    for k in (1, 2, 3):
        pl.semaphore_signal(barrier, inc=1, device_id={"sp": partner(s, k), "tp": z}, device_id_type=MESH)
    for t in range(2):
        @pl.when(z != t + 1)
        def _():
            pl.semaphore_signal(barrier, inc=1, device_id={"sp": 2 * line + 1, "tp": t + 1}, device_id_type=MESH)

    @pl.when(owner)
    def _():
        for k in (1, 2, 3):
            pl.semaphore_signal(barrier, inc=1, device_id={"sp": 2 * line, "tp": partner(z, k)}, device_id_type=MESH)
        for k in (1, 2):
            pl.semaphore_signal(barrier, inc=1, device_id={"sp": 2 * line + 1, "tp": partner(z, k)}, device_id_type=MESH)

    def remote(src, dst, send_sem, recv_sem, sp, tp):
        return pltpu.make_async_remote_copy(src_ref=src, dst_ref=dst, send_sem=send_sem, recv_sem=recv_sem,
                                            device_id={"sp": sp, "tp": tp}, device_id_type=MESH)

    loads[5].wait()
    loads[6].wait()
    sub = lax.broadcasted_iota(jnp.int32, (8, 128), 0)
    for g in range(rows // 8):
        acc = jnp.zeros((8, 128), jnp.int32)
        for r in range(8):
            acc = jnp.where(sub == r, pos_ref[8 * g + r], acc)
        posm[pl.ds(8 * g, 8), :] = acc
    angles = posm[...].astype(F32) * freq_ref[...]
    cos = jnp.cos(angles)
    sin = jnp.sin(angles)

    loads[0].wait()
    loads[1].wait()
    for r in range(rows // 16):
        wide = tok[16 * r:16 * r + 16, :].astype(F32)
        inv_rms = lax.rsqrt(jnp.mean(wide * wide, axis=-1, keepdims=True) + NORM_EPS)
        normed[16 * r:16 * r + 16, :] = (wide * inv_rms * gain[...].astype(F32).reshape(1, -1)).astype(BF16)

    def fetch(c):
        if c < chunks:
            k_loads[c].start()
            v_loads[c].start()

    def rope(lin):
        a, b = lin[:, :half], lin[:, half:]
        return jnp.concatenate([a * cos - b * sin, b * cos + a * sin], axis=-1)

    loads[2].wait()
    fetch(0)
    knew[...] = rope(jnp.dot(normed[...], wk[...], preferred_element_type=F32)).astype(BF16).astype(F32)
    loads[3].wait()
    vnew[...] = jnp.dot(normed[...], wv[...], preferred_element_type=F32).astype(BF16).astype(F32)
    loads[4].wait()
    fetch(1)
    heads = q_width // dim
    q_lin = jnp.dot(normed[...], wq[...], preferred_element_type=F32)
    q_rot = [rope(q_lin[:, h * dim:(h + 1) * dim]) for h in range(heads)]
    for g in range(rows // 8):
        qs[g] = jnp.concatenate([q_rot[h][8 * g:8 * g + 8] for h in range(heads)], axis=0).astype(BF16)

    sub16 = lax.broadcasted_iota(jnp.int32, (16, dim), 0)
    lane = lax.broadcasted_iota(jnp.int32, (16, local_slots), 1) + base
    lane128 = lax.broadcasted_iota(jnp.int32, (16, 128), 1)

    def spread_lanes(x):
        return jnp.concatenate([x] * (local_slots // 128), axis=1)

    def twice(x):
        return jnp.concatenate([x, x], axis=0)

    first = []
    for c, d in enumerate(order):
        k_loads[c].wait()
        fetch(c + 2)
        if c == chunks - 1:
            late[0].start()
            late[1].start()
        probs = []
        for u in range(CHUNK // 8):
            query = qs[2 * d + u]
            scores = jnp.zeros((16, local_slots), F32)
            for j in range(8):
                one = lax.dot_general(query, nk_ref[CHUNK * d + 8 * u + j], (((1,), (1,)), ((), ())), preferred_element_type=F32)
                scores = jnp.where(jnp.bitwise_and(sub16, 7) == j, one, scores)
            eight = pl.ds(pl.multiple_of(CHUNK * d + 8 * u, 8), 8)
            pos16 = twice(posm[eight, :])
            hit = lane == spread_lanes(jnp.bitwise_and(pos16, slots - 1))
            fresh = jnp.sum(query.astype(F32) * twice(knew[eight, :]), axis=-1, keepdims=True)
            scores = jnp.where(hit, fresh, scores) * (1.0 / math.sqrt(dim))
            valid = lane <= spread_lanes(jnp.where(pos16 >= slots - 1, slots, pos16))
            top = jnp.max(jnp.where(valid, scores, -jnp.inf), axis=-1, keepdims=True)
            safe = jnp.where(top == -jnp.inf, 0.0, top)
            weights = jnp.exp(jnp.where(valid, scores - safe, -jnp.inf))
            share = jnp.sum(weights, axis=-1, keepdims=True)
            chosen = jnp.sum(jnp.where(hit, weights, 0.0), axis=-1, keepdims=True).astype(BF16).astype(F32)
            probs.append((u, eight, jnp.where(hit, 0.0, weights).astype(BF16), chosen, top, share))
        v_loads[c].wait()
        if c == chunks - 1:
            late[2].start()
            late[3].start()
        for u, eight, weights, chosen, top, share in probs:
            out = jnp.zeros((16, dim), F32)
            for j in range(8):
                one = jnp.dot(weights, nv_ref[CHUNK * d + 8 * u + j], preferred_element_type=F32)
                out = jnp.where(jnp.bitwise_and(sub16, 7) == j, one, out)
            out = out + chosen * twice(vnew[eight, :])
            stats = jnp.where(lane128 < 64, top, share)
            for h in range(heads):
                part[chunks - 1 - c, 16 * h + 8 * u:16 * h + 8 * u + 8, 0:dim] = out[8 * h:8 * h + 8]
                part[chunks - 1 - c, 16 * h + 8 * u:16 * h + 8 * u + 8, dim:dim + 128] = stats[8 * h:8 * h + 8]
        if c == 0:
            middle = (z == 1) | (z == 2)
            pl.semaphore_wait(barrier, jnp.where(middle, jnp.where(core == 1, 9, 4), 5))
        k = chunks - 1 - c
        if k:
            first.append(remote(part.at[k], r1.at[k - 1], s1.at[k - 1], g1.at[k - 1], partner(s, k), z))
            first[-1].start()
    loads[7].wait()

    def to_owner(t, c, cut, rows, sums, send_sem, recv_sem):
        span = pl.ds(*cut[c])
        return remote(rows.at[t, :, span], sums.at[core, z, :, span], send_sem.at[t, c], recv_sem.at[core, z, c], 2 * line + 1, t + 1)

    def send_sums(value, c, cut, rows, sums, send_sem, recv_sem):
        at, size = cut[c]
        for t in range(2):
            rows[t, :, at:at + size] = value[8 * t:8 * t + 8]
        for t in range(2):
            @pl.when(jnp.logical_not(is_owner(t)))
            def _():
                to_owner(t, c, cut, rows, sums, send_sem, recv_sem).start()

    def wait_sums(c, cut, rows, sums, send_sem, recv_sem):
        at, size = cut[c]
        span = pl.ds(at, size)
        sums[1, z, :, at:at + size] = rows[tile, :, at:at + size]
        for b in range(2):
            for k in (1, 3, 2, 0):
                if b == 0 or k:
                    far = partner(z, k)
                    remote(rows.at[0, :, span], sums.at[b, far, :, span], send_sem.at[0, c], recv_sem.at[b, far, c], 2 * line + b, far).wait_recv()
        return [sums[b, 0, :, at:at + size] + sums[b, 1, :, at:at + size] + sums[b, 2, :, at:at + size] + sums[b, 3, :, at:at + size]
                for b in range(2)]

    def sent_sums(cut, rows, sums, send_sem, recv_sem):
        for t in range(2):
            @pl.when(jnp.logical_not(is_owner(t)))
            def _():
                for c in range(len(cut)):
                    to_owner(t, c, cut, rows, sums, send_sem, recv_sem).wait_send()

    for copy in first:
        copy.wait_recv()
    parts = [part[0], r1[0], r1[1], r1[2]]
    tops = [p[:, dim:dim + 1] for p in parts]
    shares = [p[:, dim + 64:dim + 65] for p in parts]
    top = jnp.maximum(jnp.maximum(tops[0], tops[1]), jnp.maximum(tops[2], tops[3]))
    scales = [jnp.exp(t - top) for t in tops]
    total = sum(f * l for f, l in zip(scales, shares))
    mixed = sum(f * p[:, :dim] for f, p in zip(scales, parts)) / total
    att = jnp.concatenate([mixed[:own_rows], mixed[own_rows:]], axis=1).astype(BF16)

    late[0].wait()
    for c, (at, size) in enumerate(CUT_O):
        send_sums(jnp.dot(att, wo[:, at:at + size], preferred_element_type=F32), c, CUT_O, y2, r2, s2, g2)

    def spread(b, k, c):
        span = pl.ds(*CUT_M[c])
        return remote(ms.at[tile, :, span] if b else norm.at[:, span], ms.at[tile, :, span], s3.at[b, k, c], g3.at[tile, c], 2 * line + b, partner(z, k))

    @pl.when(owner)
    def _():
        halves = [wait_sums(c, CUT_O, y2, r2, s2, g2) for c in range(len(CUT_O))]
        for b in range(2):
            mine = tok[pl.ds(pl.multiple_of((2 * line + b) * own_rows, own_rows), own_rows), :].astype(F32)
            mine = jnp.where(tile == 0, mine[0:8], mine[8:16])
            hidden = (mine + jnp.concatenate([h[b] for h in halves], axis=1)).astype(BF16).astype(F32)
            inv_rms = lax.rsqrt(jnp.mean(hidden * hidden, axis=-1, keepdims=True) + NORM_EPS)
            scaled = (hidden * inv_rms * gain2[...].astype(F32).reshape(1, -1)).astype(BF16).astype(F32)
            fin[line, tile, b] = hidden
            if b == 0:
                norm[...] = scaled
            else:
                ms[tile] = scaled
        for c in range(len(CUT_M)):
            for k in (2, 3, 1, 0):
                for b in (0, 1):
                    if b == 0 or k:
                        spread(b, k, c).start()

    late[1].wait()
    late[2].wait()
    gate = up = None
    for c, (at, size) in enumerate(CUT_M):
        span = pl.ds(at, size)
        for t in range(2):
            @pl.when(jnp.logical_not(is_owner(t)))
            def _():
                remote(norm.at[:, span], ms.at[t, :, span], s3.at[0, 0, c], g3.at[t, c], 2 * line + 1, t + 1).wait_recv()
        rows = jnp.concatenate([ms[0, :, at:at + size], ms[1, :, at:at + size]], axis=0).astype(BF16)
        pair = [jnp.dot(rows, w[at:at + size, :], preferred_element_type=F32) for w in (wg, wu)]
        gate = pair[0] if gate is None else gate + pair[0]
        up = pair[1] if up is None else up + pair[1]
    act = gate * (1.0 / (1.0 + jnp.exp(-gate))) * up
    act = act.astype(BF16)

    late[3].wait()
    sent_sums(CUT_O, y2, r2, s2, g2)
    for c, (at, size) in enumerate(CUT_D):
        send_sums(jnp.dot(act, wd[:, at:at + size], preferred_element_type=F32), c, CUT_D, y2, r2, s4, g4)

    def along(t, k, c):
        span = pl.ds(*CUT_D[c])
        rows = fin.at[line, t, :, :, span]
        return remote(rows, rows, s5z.at[k, c], g5z.at[t, c], s, partner(z, k))

    def across(t, c):
        span = pl.ds(*CUT_D[c])
        rows = fin.at[line, t, :, :, span]
        return remote(rows, rows, s5y.at[t, c], g5y.at[t, c], partner(s, 2), z)

    def beside(far, t, c):
        span = pl.ds(*CUT_D[c])
        rows = fin.at[line if far == 0 else 1 - line, t, :, :, span]
        return remote(rows, rows, s5c.at[far, t, c], g5c.at[far, t, c], partner(s, 1), z)

    @pl.when(owner)
    def _():
        for c, (at, size) in enumerate(CUT_D):
            totals = wait_sums(c, CUT_D, y2, r2, s4, g4)
            for b in range(2):
                fin[line, tile, b, :, at:at + size] = (fin[line, tile, b, :, at:at + size] + totals[b]).astype(BF16).astype(F32)
            for k in (2, 3, 1):
                along(tile, k, c).start()
            across(tile, c).start()
            beside(0, tile, c).start()

    @pl.when(core == 1)
    def _():
        for c in range(len(CUT_D)):
            for t in range(2):
                @pl.when(z != t + 1)
                def _():
                    along(t, 1, c).wait_recv()
                    across(t, c).start()
                    beside(0, t, c).start()
        for c in range(len(CUT_D)):
            for t in range(2):
                span = pl.ds(*CUT_D[c])
                rows = fin.at[1 - line, t, :, :, span]
                remote(rows, rows, s5y.at[t, c], g5y.at[t, c], partner(s, 2), z).wait_recv()
                beside(1, t, c).start()

    @pl.when(core == 0)
    def _():
        for far in range(2):
            for c in range(len(CUT_D)):
                for t in range(2):
                    beside(far, t, c).wait_recv()

    for y in range(2):
        for b in range(2):
            out_ref[pl.ds(own_rows * (2 * y + b), own_rows), :] = jnp.concatenate([fin[y, 0, b], fin[y, 1, b]], axis=0).astype(BF16)

    for copy in first:
        copy.wait_send()
    sent_sums(CUT_D, y2, r2, s4, g4)

    @pl.when(owner)
    def _():
        for c in range(len(CUT_M)):
            for k in range(4):
                for b in range(2):
                    if b == 0 or k:
                        spread(b, k, c).wait_send()
        for c in range(len(CUT_D)):
            for k in (1, 2, 3):
                along(tile, k, c).wait_send()

    @pl.when(core == 1)
    def _():
        for c in range(len(CUT_D)):
            for t in range(2):
                across(t, c).wait_send()
                beside(0, t, c).wait_send()
                beside(1, t, c).wait_send()


MESH = pl.DeviceIdType.MESH
CUT_O = ((0, 512), (512, 2048))
CUT_M = ((0, 512), (512, 512), (1024, 512), (1536, 512), (2048, 512))
CUT_D = ((0, 512), (512, 512), (1024, 512), (1536, 512), (2048, 512))


def layer(tokens, positions, cache_k, cache_v, gain, w_q, w_k, w_v, w_o, gain2, w_gate, w_up, w_down):
    rows, width = tokens.shape
    _, local_slots, _, dim = cache_k.shape
    heads = w_q.shape[1] // dim
    freq = (ROPE_THETA ** (-2.0 * np.arange(dim // 2, dtype=np.float64) / dim)).astype(np.float32)
    ck = cache_k.reshape(rows, local_slots, dim)
    cv = cache_v.reshape(rows, local_slots, dim)
    hbm = pl.BlockSpec(memory_space=pltpu.HBM)
    vmem = pl.BlockSpec(memory_space=pltpu.VMEM)
    dma = pltpu.SemaphoreType.DMA
    chunks = rows // CHUNK
    share = (heads * CHUNK, dim + 128)
    cut_o, cut_m, cut_d = len(CUT_O), len(CUT_M), len(CUT_D)
    return pl.pallas_call(
        layer_kernel,
        name="layer",
        out_shape=(pltpu.VMEM(ck.shape, BF16), pltpu.VMEM(cv.shape, BF16), pltpu.VMEM((rows, dim), F32),
                   pltpu.VMEM((rows, dim), F32), pltpu.VMEM((rows, width), BF16)),
        in_specs=[hbm] * 14,
        out_specs=[vmem] * 5,
        scratch_shapes=[
            pltpu.SMEM((rows,), jnp.int32),
            pltpu.VMEM((1, dim // 2), F32),
            pltpu.VMEM((rows, width), BF16),
            pltpu.VMEM((width,), BF16),
            pltpu.VMEM((width,), BF16),
            pltpu.VMEM((rows // 8, 8 * heads, dim), BF16),
            pltpu.VMEM((rows, 128), jnp.int32),
            pltpu.VMEM((chunks,) + share, F32),
            pltpu.VMEM(w_o.shape, BF16),
            pltpu.VMEM(w_gate.shape, BF16),
            pltpu.VMEM(w_up.shape, BF16),
            pltpu.VMEM(w_down.shape, BF16),
            pltpu.VMEM((3,) + share, F32),
            pltpu.VMEM((2, 8, width), F32),
            pltpu.VMEM((2, 4, 8, width), F32),
            pltpu.VMEM((8, width), F32),
            pltpu.VMEM((2, 8, width), F32),
            pltpu.VMEM((2, 2, 2, 8, width), F32),
            pltpu.VMEM((rows, width), BF16),
            dma((8,)), dma((4,)), dma((chunks,)), dma((chunks,)),
            dma((3,)), dma((3,)),
            dma((2, cut_o)), dma((2, 4, cut_o)),
            dma((2, 4, cut_m)), dma((2, cut_m)),
            dma((2, cut_d)), dma((2, 4, cut_d)),
            dma((4, cut_d)), dma((2, cut_d)),
            dma((2, cut_d)), dma((2, cut_d)),
            dma((2, 2, cut_d)), dma((2, 2, cut_d)),
        ],
        compiler_params=pltpu.CompilerParams(collective_id=0, has_side_effects=True, vmem_limit_bytes=VMEM_LAYER),
        cost_estimate=pl.CostEstimate(flops=2 * 16 * width * 2560 * 3, bytes_accessed=64 << 20, transcendentals=0),
    )(*in_hbm(positions, jnp.asarray(freq).reshape(1, -1), tokens, gain, w_q, w_k, w_v, ck, cv, gain2, w_o, w_gate, w_up, w_down))


def store_kernel(slots, pos_hbm, row_ref, knew, vnew, k_in, v_in, nk_ref, nv_ref, out_hbm, nk_hbm, nv_hbm, pos_ref, sem_p, sem_o, sem_k, sem_v):
    rows, local_slots, dim = nk_ref.shape
    base = lax.axis_index("sp") * local_slots
    fetch = pltpu.make_async_copy(pos_hbm, pos_ref, sem_p)
    fetch.start()
    out_copy = pltpu.make_async_copy(row_ref, out_hbm, sem_o)
    out_copy.start()
    sub16 = lax.broadcasted_iota(jnp.int32, (16, dim), 0)
    fetch.wait()

    def patch(ref, new_ref, b):
        offset = jnp.bitwise_and(pos_ref[b], slots - 1) - base
        inside = jnp.clip(offset, 0, local_slots - 1)
        start = pl.multiple_of((inside // 16) * 16, 16)
        old = ref[b, pl.ds(start, 16), :].astype(F32)
        ref[b, pl.ds(start, 16), :] = jnp.where(sub16 == offset - start, new_ref[pl.ds(b, 1), :], old).astype(BF16)

    stores = []
    for c in range(rows // CHUNK):
        span = pl.ds(c * CHUNK, CHUNK)
        for ref, new_ref, dst, sem in ((nk_ref, knew, nk_hbm, sem_k), (nv_ref, vnew, nv_hbm, sem_v)):
            for j in range(CHUNK):
                patch(ref, new_ref, c * CHUNK + j)
            stores.append(pltpu.make_async_copy(ref.at[span], dst.at[span], sem.at[c]))
            stores[-1].start()
    for copy in stores:
        copy.wait()
    out_copy.wait()


def store(positions, row, knew, vnew, nk, nv, slots):
    hbm = pl.BlockSpec(memory_space=pltpu.HBM)
    vmem = pl.BlockSpec(memory_space=pltpu.VMEM)
    dma = pltpu.SemaphoreType.DMA
    chunks = nk.shape[0] // CHUNK
    return pl.pallas_call(
        functools.partial(store_kernel, slots),
        name="store",
        out_shape=(pltpu.VMEM(nk.shape, BF16), pltpu.VMEM(nv.shape, BF16), jax.ShapeDtypeStruct(row.shape, BF16),
                   jax.ShapeDtypeStruct(nk.shape, BF16), jax.ShapeDtypeStruct(nv.shape, BF16)),
        in_specs=[hbm] + [vmem] * 5,
        out_specs=[vmem, vmem, hbm, hbm, hbm],
        input_output_aliases={4: 0, 5: 1},
        scratch_shapes=[pltpu.SMEM(positions.shape, jnp.int32), dma, dma, dma((chunks,)), dma((chunks,))],
        compiler_params=pltpu.CompilerParams(vmem_limit_bytes=VMEM_STORE),
    )(*in_hbm(positions), row, knew, vnew, nk, nv)[2:]


VMEM_LAYER = 48620 << 10
VMEM_STORE = 4 << 20


def solution(mesh):
    sp_size = mesh.shape["sp"]
    cache_spec = P("dp", "sp", "tp", None)
    row_spec = P("dp", None)
    col_spec = P(None, "tp")
    in_specs = (row_spec, P("dp"), cache_spec, cache_spec, P(None), col_spec, col_spec, col_spec, P("tp", None), P(None), col_spec, col_spec, P("tp", None))
    out_specs = (row_spec, cache_spec, cache_spec)

    def local_step(tokens, positions, cache_k, cache_v, attn_gain, w_q, w_k, w_v, w_o, mlp_gain, w_gate, w_up, w_down):
        nk, nv, knew, vnew, row = layer(tokens, positions, cache_k, cache_v, attn_gain, w_q, w_k, w_v, w_o, mlp_gain, w_gate, w_up, w_down)
        layer_out, new_k, new_v = store(positions, row, knew, vnew, nk, nv, sp_size * cache_k.shape[1])
        return layer_out, new_k.reshape(cache_k.shape), new_v.reshape(cache_v.shape)

    return jax.shard_map(local_step, mesh=mesh, in_specs=in_specs, out_specs=out_specs, check_vma=False)
```

```python
import functools
import math

import jax
import jax.numpy as jnp
import numpy as np
from jax import lax
from jax.experimental import pallas as pl
from jax.experimental.pallas import tpu as pltpu
from jax.sharding import PartitionSpec as P

NORM_EPS = 1e-5
ROPE_THETA = 10000.0
F32 = jnp.float32
BF16 = jnp.bfloat16
CHUNK = 16


def in_hbm(*arrays):
    return [pltpu.with_memory_space_constraint(x, pltpu.HBM) for x in arrays]


def partner(index, k):
    if k == 0:
        return index
    if k == 1:
        return index + 1 - 2 * lax.rem(index, 2)
    if k == 2:
        return lax.rem(index + 2, 4)
    return 3 - index


def layer_kernel(pos_hbm, freq_hbm, tok_hbm, gain_hbm, wq_hbm, wk_hbm, wv_hbm, ck_hbm, cv_hbm,
                 gain2_hbm, wo_hbm, wg_hbm, wu_hbm, wd_hbm, nk_ref, nv_ref, knew, vnew, out_ref, pos_ref,
                 freq_ref, tok, gain, gain2, qs, posm, part, wo, wg, wu, wd, r1, y2, r2, norm, ms, fin, normed,
                 sem_w, sem_l, sem_k, sem_v, s1, g1, s2, g2, s3, g3, s4, g4, s5z, g5z, s5y, g5y, s5c, g5c):
    s = lax.axis_index("sp")
    z = lax.axis_index("tp")
    line, core = s // 2, lax.rem(s, 2)
    width = wo.shape[1]
    own_rows = CHUNK
    rows = tok.shape[0]
    local_slots, dim = nk_ref.shape[1:]
    half = dim // 2
    chunks = rows // CHUNK
    slots = local_slots * chunks
    base = s * local_slots
    kv_width, q_width = wk_hbm.shape[1], wq_hbm.shape[1]
    wk, wv, wq = wd.at[:, 0:kv_width], wd.at[:, kv_width:2 * kv_width], wd.at[:, 2 * kv_width:2 * kv_width + q_width]
    owner = (core == 1) & ((z == 1) | (z == 2))
    tile = jnp.clip(z - 1, 0, 1)

    loads = [pltpu.make_async_copy(src, dst, sem_w.at[i]) for i, (src, dst) in enumerate((
        (tok_hbm, tok), (gain_hbm, gain), (wk_hbm, wk), (wv_hbm, wv), (wq_hbm, wq), (pos_hbm, pos_ref), (freq_hbm, freq_ref),
        (gain2_hbm, gain2)))]
    for i in (5, 6, 0, 1, 2, 3, 4, 7):
        loads[i].start()
    late = [pltpu.make_async_copy(src, dst, sem_l.at[i]) for i, (src, dst) in enumerate((
        (wo_hbm, wo), (wg_hbm, wg), (wu_hbm, wu), (wd_hbm, wd)))]
    turns = (2, 3, 1, 0)
    order = [partner(s, k) for k in turns]
    k_loads, v_loads = [], []
    for c, d in enumerate(order):
        span = pl.ds(pl.multiple_of(d * CHUNK, CHUNK), CHUNK)
        k_loads.append(pltpu.make_async_copy(ck_hbm.at[span], nk_ref.at[span], sem_k.at[c]))
        v_loads.append(pltpu.make_async_copy(cv_hbm.at[span], nv_ref.at[span], sem_v.at[c]))

    def is_owner(t):
        return (core == 1) & (z == t + 1)

    barrier = pltpu.get_barrier_semaphore()
    for k in (1, 2, 3):
        pl.semaphore_signal(barrier, inc=1, device_id={"sp": partner(s, k), "tp": z}, device_id_type=MESH)
    for t in range(2):
        @pl.when(z != t + 1)
        def _():
            pl.semaphore_signal(barrier, inc=1, device_id={"sp": 2 * line + 1, "tp": t + 1}, device_id_type=MESH)

    @pl.when(owner)
    def _():
        for k in (1, 2, 3):
            pl.semaphore_signal(barrier, inc=1, device_id={"sp": 2 * line, "tp": partner(z, k)}, device_id_type=MESH)
        for k in (1, 2):
            pl.semaphore_signal(barrier, inc=1, device_id={"sp": 2 * line + 1, "tp": partner(z, k)}, device_id_type=MESH)

    def remote(src, dst, send_sem, recv_sem, sp, tp):
        return pltpu.make_async_remote_copy(src_ref=src, dst_ref=dst, send_sem=send_sem, recv_sem=recv_sem,
                                            device_id={"sp": sp, "tp": tp}, device_id_type=MESH)

    loads[5].wait()
    loads[6].wait()
    sub = lax.broadcasted_iota(jnp.int32, (8, 128), 0)
    for g in range(rows // 8):
        acc = jnp.zeros((8, 128), jnp.int32)
        for r in range(8):
            acc = jnp.where(sub == r, pos_ref[8 * g + r], acc)
        posm[pl.ds(8 * g, 8), :] = acc
    angles = posm[...].astype(F32) * freq_ref[...]
    cos = jnp.cos(angles)
    sin = jnp.sin(angles)

    loads[0].wait()
    loads[1].wait()
    for r in range(rows // 16):
        wide = tok[16 * r:16 * r + 16, :].astype(F32)
        inv_rms = lax.rsqrt(jnp.mean(wide * wide, axis=-1, keepdims=True) + NORM_EPS)
        normed[16 * r:16 * r + 16, :] = (wide * inv_rms * gain[...].astype(F32).reshape(1, -1)).astype(BF16)

    def fetch(c):
        if c < chunks:
            k_loads[c].start()
            v_loads[c].start()

    def rope(lin):
        a, b = lin[:, :half], lin[:, half:]
        return jnp.concatenate([a * cos - b * sin, b * cos + a * sin], axis=-1)

    loads[2].wait()
    fetch(0)
    knew[...] = rope(jnp.dot(normed[...], wk[...], preferred_element_type=F32)).astype(BF16).astype(F32)
    loads[3].wait()
    vnew[...] = jnp.dot(normed[...], wv[...], preferred_element_type=F32).astype(BF16).astype(F32)
    loads[4].wait()
    fetch(1)
    heads = q_width // dim
    q_lin = jnp.dot(normed[...], wq[...], preferred_element_type=F32)
    q_rot = [rope(q_lin[:, h * dim:(h + 1) * dim]) for h in range(heads)]
    for g in range(rows // 8):
        qs[g] = jnp.concatenate([q_rot[h][8 * g:8 * g + 8] for h in range(heads)], axis=0).astype(BF16)

    sub16 = lax.broadcasted_iota(jnp.int32, (16, dim), 0)
    lane = lax.broadcasted_iota(jnp.int32, (16, local_slots), 1) + base
    lane128 = lax.broadcasted_iota(jnp.int32, (16, 128), 1)

    def spread_lanes(x):
        return jnp.concatenate([x] * (local_slots // 128), axis=1)

    def twice(x):
        return jnp.concatenate([x, x], axis=0)

    first = []
    for c, d in enumerate(order):
        k_loads[c].wait()
        fetch(c + 2)
        if c == chunks - 1:
            late[0].start()
            late[1].start()
        probs = []
        for u in range(CHUNK // 8):
            query = qs[2 * d + u]
            scores = jnp.zeros((16, local_slots), F32)
            for j in range(8):
                one = lax.dot_general(query, nk_ref[CHUNK * d + 8 * u + j], (((1,), (1,)), ((), ())), preferred_element_type=F32)
                scores = jnp.where(jnp.bitwise_and(sub16, 7) == j, one, scores)
            eight = pl.ds(pl.multiple_of(CHUNK * d + 8 * u, 8), 8)
            pos16 = twice(posm[eight, :])
            hit = lane == spread_lanes(jnp.bitwise_and(pos16, slots - 1))
            fresh = jnp.sum(query.astype(F32) * twice(knew[eight, :]), axis=-1, keepdims=True)
            scores = jnp.where(hit, fresh, scores) * (1.0 / math.sqrt(dim))
            valid = lane <= spread_lanes(jnp.where(pos16 >= slots - 1, slots, pos16))
            top = jnp.max(jnp.where(valid, scores, -jnp.inf), axis=-1, keepdims=True)
            safe = jnp.where(top == -jnp.inf, 0.0, top)
            weights = jnp.exp(jnp.where(valid, scores - safe, -jnp.inf))
            share = jnp.sum(weights, axis=-1, keepdims=True)
            chosen = jnp.sum(jnp.where(hit, weights, 0.0), axis=-1, keepdims=True).astype(BF16).astype(F32)
            probs.append((u, eight, jnp.where(hit, 0.0, weights).astype(BF16), chosen, top, share))
        v_loads[c].wait()
        if c == chunks - 1:
            late[2].start()
        for u, eight, weights, chosen, top, share in probs:
            out = jnp.zeros((16, dim), F32)
            for j in range(8):
                one = jnp.dot(weights, nv_ref[CHUNK * d + 8 * u + j], preferred_element_type=F32)
                out = jnp.where(jnp.bitwise_and(sub16, 7) == j, one, out)
            out = out + chosen * twice(vnew[eight, :])
            stats = jnp.where(lane128 < 64, top, share)
            for h in range(heads):
                part[turns[c], 16 * h + 8 * u:16 * h + 8 * u + 8, 0:dim] = out[8 * h:8 * h + 8]
                part[turns[c], 16 * h + 8 * u:16 * h + 8 * u + 8, dim:dim + 128] = stats[8 * h:8 * h + 8]
        if c == 0:
            middle = (z == 1) | (z == 2)
            pl.semaphore_wait(barrier, jnp.where(middle, jnp.where(core == 1, 9, 4), 5))
        k = turns[c]
        if k:
            first.append(remote(part.at[k], r1.at[k - 1], s1.at[k - 1], g1.at[k - 1], partner(s, k), z))
            first[-1].start()
    loads[7].wait()

    def to_owner(t, c, cut, rows, sums, send_sem, recv_sem):
        span = pl.ds(*cut[c])
        return remote(rows.at[t, :, span], sums.at[core, z, :, span], send_sem.at[t, c], recv_sem.at[core, z, c], 2 * line + 1, t + 1)

    def send_sums(value, c, cut, rows, sums, send_sem, recv_sem):
        at, size = cut[c]
        for t in range(2):
            rows[t, :, at:at + size] = value[8 * t:8 * t + 8]
        crossing = jnp.where(z < 2, 1, 0)
        for t in (crossing, 1 - crossing):
            @pl.when(jnp.logical_not(is_owner(t)))
            def _():
                to_owner(t, c, cut, rows, sums, send_sem, recv_sem).start()

    def wait_sums(c, cut, rows, sums, send_sem, recv_sem):
        at, size = cut[c]
        span = pl.ds(at, size)
        sums[1, z, :, at:at + size] = rows[tile, :, at:at + size]
        for b in range(2):
            for k in (1, 3, 2, 0):
                if b == 0 or k:
                    far = partner(z, k)
                    remote(rows.at[0, :, span], sums.at[b, far, :, span], send_sem.at[0, c], recv_sem.at[b, far, c], 2 * line + b, far).wait_recv()
        return [sums[b, 0, :, at:at + size] + sums[b, 1, :, at:at + size] + sums[b, 2, :, at:at + size] + sums[b, 3, :, at:at + size]
                for b in range(2)]

    def sent_sums(cut, rows, sums, send_sem, recv_sem):
        for t in range(2):
            @pl.when(jnp.logical_not(is_owner(t)))
            def _():
                for c in range(len(cut)):
                    to_owner(t, c, cut, rows, sums, send_sem, recv_sem).wait_send()

    for copy in first:
        copy.wait_recv()
    parts = [part[0], r1[0], r1[1], r1[2]]
    tops = [p[:, dim:dim + 1] for p in parts]
    shares = [p[:, dim + 64:dim + 65] for p in parts]
    top = jnp.maximum(jnp.maximum(tops[0], tops[1]), jnp.maximum(tops[2], tops[3]))
    scales = [jnp.exp(t - top) for t in tops]
    total = sum(f * l for f, l in zip(scales, shares))
    mixed = sum(f * p[:, :dim] for f, p in zip(scales, parts)) / total
    att = jnp.concatenate([mixed[:own_rows], mixed[own_rows:]], axis=1).astype(BF16)

    late[0].wait()
    for c, (at, size) in enumerate(CUT_O):
        send_sums(jnp.dot(att, wo[:, at:at + size], preferred_element_type=F32), c, CUT_O, y2, r2, s2, g2)

    def spread(b, k, c):
        span = pl.ds(*CUT_M[c])
        return remote(ms.at[tile, :, span] if b else norm.at[:, span], ms.at[tile, :, span], s3.at[b, k, c], g3.at[tile, c], 2 * line + b, partner(z, k))

    @pl.when(owner)
    def _():
        halves = [wait_sums(c, CUT_O, y2, r2, s2, g2) for c in range(len(CUT_O))]
        for b in range(2):
            mine = tok[pl.ds(pl.multiple_of((2 * line + b) * own_rows, own_rows), own_rows), :].astype(F32)
            mine = jnp.where(tile == 0, mine[0:8], mine[8:16])
            hidden = (mine + jnp.concatenate([h[b] for h in halves], axis=1)).astype(BF16).astype(F32)
            inv_rms = lax.rsqrt(jnp.mean(hidden * hidden, axis=-1, keepdims=True) + NORM_EPS)
            scaled = (hidden * inv_rms * gain2[...].astype(F32).reshape(1, -1)).astype(BF16).astype(F32)
            fin[line, tile, b] = hidden
            if b == 0:
                norm[...] = scaled
            else:
                ms[tile] = scaled
        for c in range(len(CUT_M)):
            for k in (2, 3, 1, 0):
                for b in (0, 1):
                    if b == 0 or k:
                        spread(b, k, c).start()

    late[1].wait()
    late[2].wait()
    late[3].start()
    gate = up = None
    for c, (at, size) in enumerate(CUT_M):
        span = pl.ds(at, size)
        for t in range(2):
            @pl.when(jnp.logical_not(is_owner(t)))
            def _():
                remote(norm.at[:, span], ms.at[t, :, span], s3.at[0, 0, c], g3.at[t, c], 2 * line + 1, t + 1).wait_recv()
        rows = jnp.concatenate([ms[0, :, at:at + size], ms[1, :, at:at + size]], axis=0).astype(BF16)
        pair = [jnp.dot(rows, w[at:at + size, :], preferred_element_type=F32) for w in (wg, wu)]
        gate = pair[0] if gate is None else gate + pair[0]
        up = pair[1] if up is None else up + pair[1]
    act = gate * (1.0 / (1.0 + jnp.exp(-gate))) * up
    act = act.astype(BF16)

    late[3].wait()
    sent_sums(CUT_O, y2, r2, s2, g2)
    for c, (at, size) in enumerate(CUT_D):
        send_sums(jnp.dot(act, wd[:, at:at + size], preferred_element_type=F32), c, CUT_D, y2, r2, s4, g4)

    def along(t, k, c):
        span = pl.ds(*CUT_D[c])
        rows = fin.at[line, t, :, :, span]
        return remote(rows, rows, s5z.at[k, c], g5z.at[t, c], s, partner(z, k))

    def across(t, c):
        span = pl.ds(*CUT_D[c])
        rows = fin.at[line, t, :, :, span]
        return remote(rows, rows, s5y.at[t, c], g5y.at[t, c], partner(s, 2), z)

    def beside(far, t, c):
        span = pl.ds(*CUT_D[c])
        rows = fin.at[line if far == 0 else 1 - line, t, :, :, span]
        return remote(rows, rows, s5c.at[far, t, c], g5c.at[far, t, c], partner(s, 1), z)

    @pl.when(owner)
    def _():
        for c, (at, size) in enumerate(CUT_D):
            totals = wait_sums(c, CUT_D, y2, r2, s4, g4)
            for b in range(2):
                fin[line, tile, b, :, at:at + size] = (fin[line, tile, b, :, at:at + size] + totals[b]).astype(BF16).astype(F32)
            for k in (2, 3, 1):
                along(tile, k, c).start()
            across(tile, c).start()
            beside(0, tile, c).start()

    @pl.when(core == 1)
    def _():
        for c in range(len(CUT_D)):
            for t in range(2):
                @pl.when(z != t + 1)
                def _():
                    along(t, 1, c).wait_recv()
                    across(t, c).start()
                    beside(0, t, c).start()
        for c in range(len(CUT_D)):
            for t in range(2):
                span = pl.ds(*CUT_D[c])
                rows = fin.at[1 - line, t, :, :, span]
                remote(rows, rows, s5y.at[t, c], g5y.at[t, c], partner(s, 2), z).wait_recv()
                beside(1, t, c).start()

    @pl.when(core == 0)
    def _():
        for far in range(2):
            for c in range(len(CUT_D)):
                for t in range(2):
                    beside(far, t, c).wait_recv()

    for y in range(2):
        for b in range(2):
            out_ref[pl.ds(own_rows * (2 * y + b), own_rows), :] = jnp.concatenate([fin[y, 0, b], fin[y, 1, b]], axis=0).astype(BF16)

    for copy in first:
        copy.wait_send()
    sent_sums(CUT_D, y2, r2, s4, g4)

    @pl.when(owner)
    def _():
        for c in range(len(CUT_M)):
            for k in range(4):
                for b in range(2):
                    if b == 0 or k:
                        spread(b, k, c).wait_send()
        for c in range(len(CUT_D)):
            for k in (1, 2, 3):
                along(tile, k, c).wait_send()

    @pl.when(core == 1)
    def _():
        for c in range(len(CUT_D)):
            for t in range(2):
                across(t, c).wait_send()
                beside(0, t, c).wait_send()
                beside(1, t, c).wait_send()


MESH = pl.DeviceIdType.MESH
CUT_O = ((0, 512), (512, 2048))
CUT_M = ((0, 256), (256, 512), (768, 768), (1536, 1024))
CUT_D = ((0, 512), (512, 512), (1024, 512), (1536, 512), (2048, 512))


def layer(tokens, positions, cache_k, cache_v, gain, w_q, w_k, w_v, w_o, gain2, w_gate, w_up, w_down):
    rows, width = tokens.shape
    _, local_slots, _, dim = cache_k.shape
    heads = w_q.shape[1] // dim
    freq = (ROPE_THETA ** (-2.0 * np.arange(dim // 2, dtype=np.float64) / dim)).astype(np.float32)
    ck = cache_k.reshape(rows, local_slots, dim)
    cv = cache_v.reshape(rows, local_slots, dim)
    hbm = pl.BlockSpec(memory_space=pltpu.HBM)
    vmem = pl.BlockSpec(memory_space=pltpu.VMEM)
    dma = pltpu.SemaphoreType.DMA
    chunks = rows // CHUNK
    share = (heads * CHUNK, dim + 128)
    cut_o, cut_m, cut_d = len(CUT_O), len(CUT_M), len(CUT_D)
    return pl.pallas_call(
        layer_kernel,
        name="layer",
        out_shape=(pltpu.VMEM(ck.shape, BF16), pltpu.VMEM(cv.shape, BF16), pltpu.VMEM((rows, dim), F32),
                   pltpu.VMEM((rows, dim), F32), pltpu.VMEM((rows, width), BF16), pltpu.SMEM((rows,), jnp.int32)),
        in_specs=[hbm] * 14,
        out_specs=[vmem] * 5 + [pl.BlockSpec(memory_space=pltpu.SMEM)],
        scratch_shapes=[
            pltpu.VMEM((1, dim // 2), F32),
            pltpu.VMEM((rows, width), BF16),
            pltpu.VMEM((width,), BF16),
            pltpu.VMEM((width,), BF16),
            pltpu.VMEM((rows // 8, 8 * heads, dim), BF16),
            pltpu.VMEM((rows, 128), jnp.int32),
            pltpu.VMEM((chunks,) + share, F32),
            pltpu.VMEM(w_o.shape, BF16),
            pltpu.VMEM(w_gate.shape, BF16),
            pltpu.VMEM(w_up.shape, BF16),
            pltpu.VMEM(w_down.shape, BF16),
            pltpu.VMEM((3,) + share, F32),
            pltpu.VMEM((2, 8, width), F32),
            pltpu.VMEM((2, 4, 8, width), F32),
            pltpu.VMEM((8, width), F32),
            pltpu.VMEM((2, 8, width), F32),
            pltpu.VMEM((2, 2, 2, 8, width), F32),
            pltpu.VMEM((rows, width), BF16),
            dma((8,)), dma((4,)), dma((chunks,)), dma((chunks,)),
            dma((3,)), dma((3,)),
            dma((2, cut_o)), dma((2, 4, cut_o)),
            dma((2, 4, cut_m)), dma((2, cut_m)),
            dma((2, cut_d)), dma((2, 4, cut_d)),
            dma((4, cut_d)), dma((2, cut_d)),
            dma((2, cut_d)), dma((2, cut_d)),
            dma((2, 2, cut_d)), dma((2, 2, cut_d)),
        ],
        compiler_params=pltpu.CompilerParams(collective_id=0, has_side_effects=True, vmem_limit_bytes=VMEM_LAYER),
        cost_estimate=pl.CostEstimate(flops=2 * 16 * width * 2560 * 3, bytes_accessed=64 << 20, transcendentals=0),
    )(*in_hbm(positions, jnp.asarray(freq).reshape(1, -1), tokens, gain, w_q, w_k, w_v, ck, cv, gain2, w_o, w_gate, w_up, w_down))


def store_kernel(slots, pos_ref, row_ref, knew, vnew, k_in, v_in, nk_ref, nv_ref, out_hbm, nk_hbm, nv_hbm, sem_o, sem_k, sem_v):
    rows, local_slots, dim = nk_ref.shape
    base = lax.axis_index("sp") * local_slots
    out_copy = pltpu.make_async_copy(row_ref, out_hbm, sem_o)
    out_copy.start()
    sub16 = lax.broadcasted_iota(jnp.int32, (16, dim), 0)

    def patch(ref, new_ref, b):
        offset = jnp.bitwise_and(pos_ref[b], slots - 1) - base
        inside = jnp.clip(offset, 0, local_slots - 1)
        start = pl.multiple_of((inside // 16) * 16, 16)
        old = ref[b, pl.ds(start, 16), :].astype(F32)
        ref[b, pl.ds(start, 16), :] = jnp.where(sub16 == offset - start, new_ref[pl.ds(b, 1), :], old).astype(BF16)

    stores = []
    for c in range(rows // CHUNK):
        span = pl.ds(c * CHUNK, CHUNK)
        for ref, new_ref, dst, sem in ((nk_ref, knew, nk_hbm, sem_k), (nv_ref, vnew, nv_hbm, sem_v)):
            for j in range(CHUNK):
                patch(ref, new_ref, c * CHUNK + j)
            stores.append(pltpu.make_async_copy(ref.at[span], dst.at[span], sem.at[c]))
            stores[-1].start()
    for copy in stores:
        copy.wait()
    out_copy.wait()


def store(places, row, knew, vnew, nk, nv, slots):
    hbm = pl.BlockSpec(memory_space=pltpu.HBM)
    vmem = pl.BlockSpec(memory_space=pltpu.VMEM)
    dma = pltpu.SemaphoreType.DMA
    chunks = nk.shape[0] // CHUNK
    return pl.pallas_call(
        functools.partial(store_kernel, slots),
        name="store",
        out_shape=(pltpu.VMEM(nk.shape, BF16), pltpu.VMEM(nv.shape, BF16), jax.ShapeDtypeStruct(row.shape, BF16),
                   jax.ShapeDtypeStruct(nk.shape, BF16), jax.ShapeDtypeStruct(nv.shape, BF16)),
        in_specs=[pl.BlockSpec(memory_space=pltpu.SMEM)] + [vmem] * 5,
        out_specs=[vmem, vmem, hbm, hbm, hbm],
        input_output_aliases={4: 0, 5: 1},
        scratch_shapes=[dma, dma((chunks,)), dma((chunks,))],
        compiler_params=pltpu.CompilerParams(vmem_limit_bytes=VMEM_STORE),
    )(places, row, knew, vnew, nk, nv)[2:]


VMEM_LAYER = 48620 << 10
VMEM_STORE = 4 << 20


def solution(mesh):
    sp_size = mesh.shape["sp"]
    cache_spec = P("dp", "sp", "tp", None)
    row_spec = P("dp", None)
    col_spec = P(None, "tp")
    in_specs = (row_spec, P("dp"), cache_spec, cache_spec, P(None), col_spec, col_spec, col_spec, P("tp", None), P(None), col_spec, col_spec, P("tp", None))
    out_specs = (row_spec, cache_spec, cache_spec)

    def local_step(tokens, positions, cache_k, cache_v, attn_gain, w_q, w_k, w_v, w_o, mlp_gain, w_gate, w_up, w_down):
        nk, nv, knew, vnew, row, places = layer(tokens, positions, cache_k, cache_v, attn_gain, w_q, w_k, w_v, w_o, mlp_gain, w_gate, w_up, w_down)
        layer_out, new_k, new_v = store(places, row, knew, vnew, nk, nv, sp_size * cache_k.shape[1])
        return layer_out, new_k.reshape(cache_k.shape), new_v.reshape(cache_v.shape)

    return jax.shard_map(local_step, mesh=mesh, in_specs=in_specs, out_specs=out_specs, check_vma=False)
```
